8 devices in a mesh: dp: 2 (over z, y), ep: 4 (over x, core).
Axes of the slice: x: 2, y: 2, z: 1, core: 2. Of those that a mesh axis runs over, the one named last changes fastest.
Arguments:
- x_rows: bfloat16 [4096, 2048], P(('dp', 'ep')), parts along dimension 0
- sel_idx: int32 [128, 32], P(('dp', 'ep')), parts along dimension 0
- gate_w: float32 [128, 32], P(('dp', 'ep')), parts along dimension 0
- w_up: bfloat16 [64, 2048, 1024], P('ep')
- w_down: bfloat16 [64, 1024, 2048], P('ep')
Outputs:
- output: bfloat16 [4096, 2048], P(('dp', 'ep')), parts along dimension 0
There are 2 independent parts. The reference program is written for one: setup_inputs(seed, part) draws one part's arguments, and reference() takes and returns one part's arrays. A program takes and returns all parts, laid end to end along the dimension named above; an argument that names none is the same for every part.
All inputs are finite; a program needn't handle non-finite values.
Results may differ from the reference program's by a relative error of at most 0.001.
Values are sent between devices in bfloat16 or wider.
A program may use at most 1 GiB of HBM per device.

```python
import jax
import jax.numpy as jnp
from jax import lax

D_MODEL = 2048
D_FF = 1024
EXPERTS = 64
GROUP_SIZE = 4
TOKENS = 2048
CAPACITY = 32

TOK_LOC = TOKENS // GROUP_SIZE
EXP_LOC = EXPERTS // GROUP_SIZE
PER_SOURCE = CAPACITY // GROUP_SIZE


def draw_selection(sel_key):
    key_order, key_hot, key_rank, key_delta, key_rows, key_cols = jax.random.split(sel_key, 6)
    dev_order = jax.random.permutation(key_order, GROUP_SIZE)
    hot_owner = dev_order[jax.random.randint(key_hot, (GROUP_SIZE,), 0, max(1, GROUP_SIZE // 4))]
    hot_expert = jnp.repeat(hot_owner, EXP_LOC)
    rank_keys = jax.random.randint(key_rank, (EXPERTS, GROUP_SIZE), 0, 1048576)
    rank_keys = jnp.where(jnp.arange(GROUP_SIZE)[None, :] == hot_expert[:, None], -1, rank_keys)
    src_order = jnp.argsort(rank_keys, axis=1, stable=True)
    delta_rows = jax.random.randint(key_delta, (EXPERTS, (GROUP_SIZE - 2) // 2), 0, PER_SOURCE + 1)
    paired = jnp.stack([PER_SOURCE + delta_rows, PER_SOURCE - delta_rows], axis=2).reshape(EXPERTS, GROUP_SIZE - 2)
    count_by_pos = jnp.concatenate([jnp.full((EXPERTS, 1), 2 * PER_SOURCE, jnp.int32), paired.astype(jnp.int32), jnp.zeros((EXPERTS, 1), jnp.int32)], axis=1)
    count_dev = jnp.take_along_axis(count_by_pos, jnp.argsort(src_order, axis=1), axis=1)
    row_ends = jnp.cumsum(count_dev, axis=1)
    row_starts = row_ends - count_dev
    slot_ids = jnp.arange(CAPACITY)
    source = jnp.sum((row_ends[:, None, :] <= slot_ids[None, :, None]).astype(jnp.int32), axis=2)
    rank_in = slot_ids[None, :] - jnp.take_along_axis(row_starts, source, axis=1)
    row_perm = jnp.argsort(jax.random.bits(key_rows, (EXPERTS, GROUP_SIZE, TOK_LOC)), axis=2).reshape(EXPERTS, TOKENS)
    picked = jnp.take_along_axis(row_perm, source * TOK_LOC + rank_in, axis=1)
    tokens = source * TOK_LOC + picked
    col_perm = jnp.argsort(jax.random.bits(key_cols, (EXPERTS, CAPACITY)), axis=1)
    return jnp.take_along_axis(tokens, col_perm, axis=1).astype(jnp.int32)


def setup_inputs(seed: int = 0, part: int = 0) -> dict:
    base_key = jax.random.key(seed)
    part_key = jax.random.fold_in(base_key, part)
    key_x, key_sel, key_gate = jax.random.split(part_key, 3)
    key_up, key_down = jax.random.split(jax.random.key(seed + 1), 2)
    up_scale = D_MODEL ** -0.5
    down_scale = 1.5 * D_FF ** -0.5
    x_rows = jax.random.normal(key_x, (TOKENS, D_MODEL), jnp.float32).astype(jnp.bfloat16)
    sel_idx = draw_selection(key_sel)
    gate_w = jax.random.uniform(key_gate, (EXPERTS, CAPACITY), jnp.float32, 0.25, 1.25)
    w_up = (jax.random.normal(key_up, (EXPERTS, D_MODEL, D_FF), jnp.float32) * up_scale).astype(jnp.bfloat16)
    w_down = (jax.random.normal(key_down, (EXPERTS, D_FF, D_MODEL), jnp.float32) * down_scale).astype(jnp.bfloat16)
    return {"x_rows": x_rows, "sel_idx": sel_idx, "gate_w": gate_w, "w_up": w_up, "w_down": w_down}


def reference(x_rows, sel_idx, gate_w, w_up, w_down):
    def one_expert(expert_args):
        sel_row, gate_row, up_mat, down_mat = expert_args
        chosen = jnp.take(x_rows, sel_row, axis=0)
        hidden = jax.nn.gelu(jnp.dot(chosen, up_mat, preferred_element_type=jnp.float32), approximate=True).astype(jnp.bfloat16)
        out_rows = jnp.dot(hidden, down_mat, preferred_element_type=jnp.float32)
        return (out_rows * gate_row[:, None]).astype(jnp.bfloat16)

    contrib = lax.map(one_expert, (sel_idx, gate_w, w_up, w_down))
    summed = jax.ops.segment_sum(contrib.reshape(EXPERTS * CAPACITY, D_MODEL).astype(jnp.float32), sel_idx.reshape(EXPERTS * CAPACITY), num_segments=TOKENS)
    return (x_rows.astype(jnp.float32) + summed).astype(jnp.bfloat16)
```

```python
import functools

import jax
import jax.numpy as jnp
from jax import lax
from jax.experimental import pallas as pl
from jax.experimental.pallas import tpu as pltpu
from jax.sharding import PartitionSpec as P

MESH = pl.DeviceIdType.MESH
CHUNKS = 4
RING = 3


def moe_kernel(sel_col, slot_of, gate_of, tab, x_hbm, up_hbm, down_hbm, y_ref,
               x_all, picked, hot, acc, outbox, inbox, tabs, up_buf, down_buf,
               x_sem, up_sem, down_sem, send_link, recv_link, send_fwd, recv_fwd, send_near, recv_near,
               send_tab, recv_tab, send_ret, recv_ret):
    tok, width = y_ref.shape
    experts = slot_of.shape[0]
    cap = slot_of.shape[1]
    part = cap // 2
    half = experts // 2
    rows = tok // CHUNKS
    me = lax.axis_index("ep")
    near = me + 1 - 2 * (me % 2)
    far = (me + 2) % 4
    diag = 3 - me
    peers = (near, far, diag)
    chip = me // 2
    own = pl.multiple_of(me * tok, tok)

    def up_copy(e):
        return pltpu.make_async_copy(up_hbm.at[e], up_buf.at[e % RING], up_sem.at[e % RING])

    def down_copy(e):
        return pltpu.make_async_copy(down_hbm.at[e], down_buf.at[e % RING], down_sem.at[e % RING])

    def remote(src, dst, send, recv, peer):
        return pltpu.make_async_remote_copy(src_ref=src, dst_ref=dst, send_sem=send, recv_sem=recv,
                                            device_id={"ep": peer}, device_id_type=MESH)

    load_x = pltpu.make_async_copy(x_hbm, x_all.at[pl.ds(own, tok)], x_sem)
    load_x.start()
    for e in range(RING):
        up_copy(e).start()
        down_copy(e).start()

    barrier = pltpu.get_barrier_semaphore()
    for peer in peers:
        pl.semaphore_signal(barrier, inc=1, device_id={"ep": peer}, device_id_type=MESH)
    pl.semaphore_wait(barrier, 3)

    def chunk_at(dev, c):
        return x_all.at[pl.ds(pl.multiple_of(dev * tok + c * rows, rows), rows)]

    load_x.wait()
    link = [remote(chunk_at(me, c), chunk_at(me, c), send_link.at[c], recv_link.at[c], far) for c in range(CHUNKS)]
    for copy in link:
        copy.start()
    whole = x_all.at[pl.ds(own, tok)]
    to_near = remote(whole, whole, send_near, recv_near, near)
    to_near.start()
    table = [remote(tab.at[peer], tabs.at[me], send_tab.at[i], recv_tab.at[i], peer) for i, peer in enumerate(peers)]
    for copy in table:
        copy.start()
    tabs[me] = tab[me]
    acc[...] = x_all[pl.ds(own, tok), :].astype(jnp.float32)

    def pick(start, size, first):
        col = lax.broadcasted_iota(jnp.int32, (experts * cap, size), 1) + start
        hot[:, 0:size] = jnp.where(sel_col[...] == col, 1.0, 0.0).astype(jnp.bfloat16)

        @pl.loop(0, width // 256)
        def _(n):
            cols = pl.ds(pl.multiple_of(n * 256, 256), 256)
            got = jnp.dot(hot[:, 0:size], x_all[pl.ds(pl.multiple_of(start, size), size), cols],
                          preferred_element_type=jnp.float32).astype(jnp.bfloat16)
            if first:
                picked[:, cols] = got
            else:
                picked[:, cols] = picked[:, cols] + got

    pick(own, tok, True)
    to_near.wait()
    pick(near * tok, tok, False)
    forward = [remote(chunk_at(far, c), chunk_at(far, c), send_fwd.at[c], recv_fwd.at[c], near) for c in range(CHUNKS)]
    for c in range(CHUNKS):
        link[c].wait_recv()
        forward[c].start()
        pick(far * tok + c * rows, rows, False)
        forward[c].wait_recv()
        pick(diag * tok + c * rows, rows, False)

    def one_hot_t(h, pair):
        idx = jnp.concatenate([tabs[pair * 2, h], tabs[pair * 2 + 1, h]], axis=1)
        row = lax.broadcasted_iota(jnp.int32, (tok, idx.shape[1]), 0)
        hot[:, 0:idx.shape[1]] = jnp.where(row == idx, 1.0, 0.0).astype(jnp.bfloat16)

    def add_pair(h, pair):
        one_hot_t(h, pair)
        depth = 2 * half * part

        @pl.loop(0, width // 256)
        def _(n):
            cols = pl.ds(pl.multiple_of(n * 256, 256), 256)
            acc[:, cols] += jnp.dot(hot[:, 0:depth], inbox[h, pl.ds(pair * depth, depth), cols],
                                    preferred_element_type=jnp.float32)

    def from_peer(i, h):
        block = inbox.at[h, pl.ds(pl.multiple_of(peers[i] * half * part, half * part), half * part)]
        return remote(block, block, send_ret.at[i, h], recv_ret.at[i, h], peers[i])

    def expert(e, carry):
        h = e // half
        up_copy(e).wait()
        z = jnp.dot(picked[pl.ds(pl.multiple_of(e * cap, cap), cap), :], up_buf[e % RING],
                    preferred_element_type=jnp.float32)
        act = (0.5 * z * (1.0 + jnp.tanh(0.7978845608028654 * (z + 0.044715 * (z * z * z))))).astype(jnp.bfloat16)

        @pl.when(e + RING < experts)
        def _():
            up_copy(e + RING).start()

        place = slot_of[pl.ds(e, 1), :] == lax.broadcasted_iota(jnp.int32, (4 * part, cap), 0)
        perm = jnp.where(place, 1.0, 0.0)
        gate = jnp.sum(perm * gate_of[pl.ds(e, 1), :], axis=1, keepdims=True)
        act = jnp.dot(perm.astype(jnp.bfloat16), act, preferred_element_type=jnp.float32).astype(jnp.bfloat16)
        down_copy(e).wait()
        for n in range(width // 512):
            cols = slice(n * 512, (n + 1) * 512)
            o = jnp.dot(act, down_buf[e % RING, :, cols], preferred_element_type=jnp.float32)
            outbox[e, :, cols] = (o * gate).astype(jnp.bfloat16)

        @pl.when(e + RING < experts)
        def _():
            down_copy(e + RING).start()

        spot = pl.ds(pl.multiple_of(me * half * part + (e % half) * part, part), part)
        for i in (1, 2, 0):
            remote(outbox.at[e, pl.ds(pl.multiple_of(peers[i] * part, part), part)], inbox.at[h, spot],
                   send_ret.at[i, h], recv_ret.at[i, h], peers[i]).start()
        inbox[h, spot, :] = outbox[e, pl.ds(pl.multiple_of(me * part, part), part), :]

        @pl.when(e == experts - 3)
        def _():
            for copy in table:
                copy.wait()
            for i in range(3):
                from_peer(i, 0).wait_recv()
            add_pair(0, 0)
            add_pair(0, 1)
        return carry

    lax.fori_loop(0, experts, expert, 0)
    from_peer(0, 1).wait_recv()
    add_pair(1, chip)
    from_peer(1, 1).wait_recv()
    from_peer(2, 1).wait_recv()
    add_pair(1, 1 - chip)
    y_ref[...] = acc[...].astype(jnp.bfloat16)

    for c in range(CHUNKS):
        link[c].wait_send()
        forward[c].wait_send()
    for h in range(2):
        for i in range(3):
            from_peer(i, h).wait_send()


def solution(mesh):
    group_size = mesh.shape["ep"]

    def local_layer(x_loc, sel_loc, gate_loc, up_loc, down_loc):
        tok, width = x_loc.shape
        experts, cap = sel_loc.shape
        hidden = up_loc.shape[2]
        part = cap // 2
        owner = sel_loc // tok
        local_row = sel_loc - owner * tok
        same = owner[:, :, None] == owner[:, None, :]
        before = jnp.arange(cap)[None, :, None] > jnp.arange(cap)[None, None, :]
        rank = jnp.sum((same & before).astype(jnp.int32), axis=2)
        slot = owner * part + rank
        hit = slot[:, None, :] == jnp.arange(group_size * part)[None, :, None]
        tab = jnp.max(jnp.where(hit, local_row[:, None, :], -1), axis=2)
        tab = tab.reshape(experts, group_size, part).transpose(1, 0, 2).reshape(group_size, 2, 1, experts * part // 2)
        sel_col = sel_loc.reshape(experts * cap, 1)
        vmem = pl.BlockSpec(memory_space=pltpu.VMEM)
        hbm = pl.BlockSpec(memory_space=pl.ANY)
        bf16 = jnp.bfloat16
        dma = pltpu.SemaphoreType.DMA
        return pl.pallas_call(
            moe_kernel,
            out_shape=jax.ShapeDtypeStruct((tok, width), bf16),
            in_specs=[vmem, vmem, vmem, vmem, hbm, hbm, hbm],
            out_specs=vmem,
            scratch_shapes=[
                pltpu.VMEM((group_size * tok, width), bf16),
                pltpu.VMEM((experts * cap, width), bf16),
                pltpu.VMEM((tok, tok), bf16),
                pltpu.VMEM((tok, width), jnp.float32),
                pltpu.VMEM((experts, group_size * part, width), bf16),
                pltpu.VMEM((2, group_size * experts * part // 2, width), bf16),
                pltpu.VMEM(tab.shape, jnp.int32),
                pltpu.VMEM((RING, width, hidden), bf16),
                pltpu.VMEM((RING, hidden, width), bf16),
                dma, dma((RING,)), dma((RING,)),
                dma((CHUNKS,)), dma((CHUNKS,)), dma((CHUNKS,)), dma((CHUNKS,)), dma, dma,
                dma((3,)), dma((3,)), dma((3, 2)), dma((3, 2)),
            ],
            compiler_params=pltpu.CompilerParams(collective_id=0, has_side_effects=True,
                                                 vmem_limit_bytes=64 * 1024 * 1024 - 65536),
        )(sel_col, slot, gate_loc, tab, x_loc, up_loc, down_loc)

    row_spec = P(("dp", "ep"), None)
    weight_spec = P("ep", None, None)
    return jax.shard_map(local_layer, mesh=mesh, in_specs=(row_spec, row_spec, row_spec, weight_spec, weight_spec), out_specs=row_spec, check_vma=False)
```

```python
import functools

import jax
import jax.numpy as jnp
from jax import lax
from jax.experimental import pallas as pl
from jax.experimental.pallas import tpu as pltpu
from jax.sharding import PartitionSpec as P

MESH = pl.DeviceIdType.MESH
RING = 3
GROUPS = 4
LANES = 128
BF16 = jnp.bfloat16
F32 = jnp.float32
I32 = jnp.int32


def iota(shape, dim):
    return lax.broadcasted_iota(I32, shape, dim)


def mm(a, b):
    return jnp.dot(a.astype(BF16), b.astype(BF16), preferred_element_type=F32)


def mm_t(a, b):
    return lax.dot_general(a.astype(BF16), b.astype(BF16), (((1,), (1,)), ((), ())), preferred_element_type=F32)


def flag(cond):
    return jnp.where(cond, 1.0, 0.0)


def total(a):
    return jnp.sum(jnp.sum(a, axis=1, keepdims=True), axis=0, keepdims=True)


def moe_kernel(xcap, rcap, checked, sel_in, gate_in, x_hbm, up_hbm, down_hbm, y_ref, ok_ref,
               x_chip, x_out, x_in, picked, contrib, contrib_near, ret_out, ret_in, acc, hot,
               sels, slots, toks, sel_col, gate_col, need_col, pos_out, square, ok_mine, ok_other, up_buf, down_buf,
               x_sem, up_sem, down_sem, send_sel, recv_sel, send_x, recv_x, send_link, recv_link, send_fwd, recv_fwd,
               send_near, recv_near, send_ret, recv_ret, send_back, recv_back, send_ok, recv_ok):
    tok, width = y_ref.shape
    cap = 32
    experts = GROUPS * LANES // cap
    per_group = experts // GROUPS
    xoff = [sum(xcap[:i]) for i in range(GROUPS + 1)]
    roff = [sum(rcap[:i]) for i in range(GROUPS + 1)]
    me = lax.axis_index("ep")
    core = me % 2
    chip = me // 2
    near = me + 1 - 2 * core
    far = (me + 2) % 4
    diag = 3 - me
    peers = (near, far, diag)
    other_group = 1 - lax.axis_index("dp")

    def up_copy(e):
        return pltpu.make_async_copy(up_hbm.at[e], up_buf.at[e % RING], up_sem.at[e % RING])

    def down_copy(e):
        return pltpu.make_async_copy(down_hbm.at[e], down_buf.at[e % RING], down_sem.at[e % RING])

    def remote(src, dst, send, recv, peer, axis="ep"):
        return pltpu.make_async_remote_copy(src_ref=src, dst_ref=dst, send_sem=send, recv_sem=recv,
                                            device_id={axis: peer}, device_id_type=MESH)

    own_rows = pl.ds(pl.multiple_of(core * tok, tok), tok)
    near_rows = pl.ds(pl.multiple_of((1 - core) * tok, tok), tok)
    load_x = pltpu.make_async_copy(x_hbm, x_chip.at[own_rows], x_sem)
    load_x.start()

    barrier = pltpu.get_barrier_semaphore()
    for peer in peers:
        pl.semaphore_signal(barrier, inc=1, device_id={"ep": peer}, device_id_type=MESH)
    if checked:
        pl.semaphore_signal(barrier, inc=1, device_id={"dp": other_group}, device_id_type=MESH)
    for e in range(RING):
        up_copy(e).start()
        down_copy(e).start()
    pl.semaphore_wait(barrier, 4 if checked else 3)

    sel_send = [remote(sel_in, sels.at[me], send_sel.at[i], recv_sel.at[i], peer) for i, peer in enumerate(peers)]
    for copy in sel_send:
        copy.start()
    load_x.wait()
    to_near = remote(x_chip.at[own_rows], x_chip.at[own_rows], send_x, recv_x, near)
    to_near.start()
    sels[me] = sel_in[...]

    square[...] = jnp.zeros_like(square)
    square[0:GROUPS, :] = sel_in[...].astype(F32)
    square[8:8 + GROUPS, :] = gate_in[...]
    turned = square[...].T
    for j in range(GROUPS):
        sel_col[j * LANES:(j + 1) * LANES, :] = turned[:, j:j + 1].astype(I32)
        gate_col[j * LANES:(j + 1) * LANES, :] = turned[:, 8 + j:9 + j]
    for copy in sel_send:
        copy.wait_recv()

    before = flag(iota((LANES, LANES), 0) < iota((LANES, LANES), 1))
    ones = jnp.ones((LANES, LANES), F32)
    rows_before = flag(iota((GROUPS * 8, GROUPS * 8), 1) < iota((GROUPS * 8, GROUPS * 8), 0))

    def row_order(c):
        base = (1 - c) * (2 * tok)
        seen = jnp.zeros((8, LANES), F32)
        firsts, fits = [], []
        for j in range(GROUPS):
            row = jnp.concatenate([sels[2 * c, j:j + 1, :], sels[2 * c + 1, j:j + 1, :]], axis=1) - base
            high = flag(iota((8, 2 * LANES), 0) == (row >> 7))
            low = flag(iota((LANES, 2 * LANES), 0) == (row & 127))
            need = flag(mm_t(high, low) > 0.5)
            firsts.append(need * (1.0 - seen))
            seen = jnp.maximum(seen, need)
            fits.append(flag(total(seen) < xoff[j + 1] + 0.5))
        first = jnp.concatenate(firsts, axis=0)
        place = mm(first, before) + mm(rows_before, mm(first, ones))
        pos = sum(firsts[j] * (place[8 * j:8 * j + 8] + 1.0) for j in range(GROUPS)) - 1.0
        return pos, fits[0] * fits[1] * fits[2] * fits[3]

    def entry_order(d):
        away = flag((sels[d] >> 10) != d // 2)
        rank = mm(away, before)
        count = jnp.sum(away, axis=1, keepdims=True)
        end = jnp.zeros((1, 1), F32)
        for j in range(GROUPS):
            begin = jnp.maximum(end, float(roff[j]))
            slots[d, j:j + 1, :] = (away[j:j + 1] * (rank[j:j + 1] + begin + 1.0) - 1.0).astype(I32)
            end = begin + count[j:j + 1]
        return flag(end < roff[GROUPS] + 0.5)

    to_send, fit = row_order(1 - chip)
    pos_out[...] = to_send.astype(I32)
    to_near.wait_recv()

    link = []
    for i in range(GROUPS):
        part = xcap[i] // 2
        start = xoff[i] + core * part
        for b in range(8):
            hot[0:part, b * LANES:(b + 1) * LANES] = flag(iota((part, LANES), 0) + start == pos_out[b:b + 1, :]).astype(BF16)
        at = pl.ds(xoff[i] // 2, part)

        @pl.loop(0, width // 256)
        def _(n):
            cols = pl.ds(pl.multiple_of(n * 256, 256), 256)
            x_out[at, cols] = jnp.dot(hot[0:part, 0:2 * tok], x_chip[:, cols], preferred_element_type=F32).astype(BF16)

        link.append(remote(x_out.at[at], x_in.at[pl.ds(pl.multiple_of(start, 16), part)], send_link.at[i], recv_link.at[i], far))
        link[i].start()

    wanted, fit_in = row_order(chip)
    fit = fit * fit_in
    for d in range(4):
        fit = fit * entry_order(d)

    found = jnp.zeros((GROUPS * LANES, LANES), F32)
    for b in range(8):
        base = (1 - chip) * (2 * tok) + b * LANES
        found = found + jnp.where(sel_col[...] == iota((GROUPS * LANES, LANES), 1) + base, wanted[b:b + 1, :] + 1.0, 0.0)
    need_col[...] = (jnp.sum(found, axis=1, keepdims=True) - 1.0).astype(I32)

    for b in range(8):
        base = chip * (2 * tok) + b * LANES
        hot[:, b * LANES:(b + 1) * LANES] = flag(sel_col[...] == iota((GROUPS * LANES, LANES), 1) + base).astype(BF16)

    @pl.loop(0, width // 256)
    def _(n):
        cols = pl.ds(pl.multiple_of(n * 256, 256), 256)
        picked[:, cols] = jnp.dot(hot[:, 0:2 * tok], x_chip[:, cols], preferred_element_type=F32).astype(BF16)

    for f, d in enumerate((far, diag)):
        row = sels[d]
        for j in range(GROUPS):
            sums = jnp.zeros((8, LANES), F32)
            for k in range(j + 1):
                chosen = flag(iota((LANES, LANES), 0) + roff[j] == slots[d, k:k + 1, :])
                at = iota((8, LANES), 0)
                value = jnp.where(at == 0, row[k:k + 1] >> 5, jnp.where(at == 1, row[k:k + 1] & 31, 1)).astype(F32)
                sums = sums + mm_t(value, chosen)
            token = jnp.where((sums[2:3] > 0.5) & (iota((1, LANES), 1) < rcap[j]), sums[0:1] * 32.0 + sums[1:2], -1.0)
            toks[f, j] = token.astype(I32)

    if checked:
        ok_mine[...] = jnp.broadcast_to(fit, ok_mine.shape)
        ok_send = remote(ok_mine, ok_other, send_ok, recv_ok, other_group, "dp")
        ok_send.start()

    acc[...] = x_chip[own_rows, :].astype(F32)

    forward = []
    for i in range(GROUPS):
        part = xcap[i] // 2
        block = x_in.at[pl.ds(pl.multiple_of(xoff[i] + core * part, 16), part)]
        forward.append(remote(block, block, send_fwd.at[i], recv_fwd.at[i], near))

    def arrive(i):
        link[i].wait_recv()
        forward[i].start()
        r0, size = i * LANES, xcap[i]
        hot[r0:, 0:size] = flag(need_col[r0:, :] == iota((GROUPS * LANES - r0, size), 1) + xoff[i]).astype(BF16)
        forward[i].wait_recv()

        @pl.loop(0, width // 256)
        def _(n):
            cols = pl.ds(pl.multiple_of(n * 256, 256), 256)
            picked[r0:, cols] = picked[r0:, cols] + jnp.dot(
                hot[r0:, 0:size], x_in[xoff[i]:xoff[i + 1], cols], preferred_element_type=F32).astype(BF16)

    pass_near, back = [], []
    for j in range(GROUPS):
        block = pl.ds(j * LANES, LANES)
        pass_near.append(remote(contrib.at[block], contrib_near.at[block], send_near.at[j], recv_near.at[j], near))
        block = pl.ds(roff[j], rcap[j])
        back.append(remote(ret_out.at[block], ret_in.at[0, block], send_ret.at[j], recv_ret.at[j], far))

    def give(j):
        pass_near[j].start()
        depth = (j + 1) * LANES
        for k in range(j + 1):
            hot[0:rcap[j], k * LANES:(k + 1) * LANES] = flag(
                iota((rcap[j], LANES), 0) + roff[j] == slots[me, k:k + 1, :]).astype(BF16)

        @pl.loop(0, width // 256)
        def _(n):
            cols = pl.ds(pl.multiple_of(n * 256, 256), 256)
            ret_out[roff[j]:roff[j + 1], cols] = jnp.dot(
                hot[0:rcap[j], 0:depth], contrib[0:depth, cols], preferred_element_type=F32).astype(BF16)

        back[j].start()

    def expert(e, carry):
        for i in range(GROUPS):
            pl.when(e == i * per_group)(functools.partial(arrive, i))
        rows = pl.ds(pl.multiple_of(e * cap, cap), cap)
        up_copy(e).wait()
        z = jnp.dot(picked[rows, :], up_buf[e % RING], preferred_element_type=F32)
        act = (0.5 * z * (1.0 + jnp.tanh(0.7978845608028654 * (z + 0.044715 * (z * z * z))))).astype(BF16)

        @pl.when(e + RING < experts)
        def _():
            up_copy(e + RING).start()

        down_copy(e).wait()
        for n in range(width // 512):
            cols = slice(n * 512, (n + 1) * 512)
            o = jnp.dot(act, down_buf[e % RING, :, cols], preferred_element_type=F32)
            contrib[rows, cols] = (o * gate_col[rows, :]).astype(BF16)

        @pl.when(e + RING < experts)
        def _():
            down_copy(e + RING).start()

        for j in range(GROUPS):
            pl.when(e == j * per_group + per_group - 1)(functools.partial(give, j))
        return carry

    lax.fori_loop(0, experts, expert, 0)

    def add_rows(d, source):
        for j in range(GROUPS):
            hot[:, j * LANES:(j + 1) * LANES] = flag(iota((tok, LANES), 0) + me * tok == sels[d, j:j + 1, :]).astype(BF16)

        @pl.loop(0, width // 256)
        def _(n):
            cols = pl.ds(pl.multiple_of(n * 256, 256), 256)
            acc[:, cols] += jnp.dot(hot[:, 0:GROUPS * LANES], source[:, cols], preferred_element_type=F32)

    def add_back(f, j):
        hot[:, 0:LANES] = flag(iota((tok, LANES), 0) + me * tok == toks[f, j]).astype(BF16)

        @pl.loop(0, width // 256)
        def _(n):
            cols = pl.ds(pl.multiple_of(n * 256, 256), 256)
            acc[:, cols] += jnp.dot(hot[:, 0:rcap[j]], ret_in[f, roff[j]:roff[j + 1], cols], preferred_element_type=F32)

    again = []
    for j in range(GROUPS):
        block = pl.ds(roff[j], rcap[j])
        again.append(remote(ret_in.at[0, block], ret_in.at[1, block], send_back.at[j], recv_back.at[j], near))

    add_rows(me, contrib)
    for j in range(GROUPS):
        pass_near[j].wait_recv()
    add_rows(near, contrib_near)
    for j in range(GROUPS):
        back[j].wait_recv()
        again[j].start()
        add_back(0, j)
        again[j].wait_recv()
        add_back(1, j)
    y_ref[...] = acc[...].astype(BF16)

    if checked:
        ok_send.wait()
        ok_ref[...] = ok_mine[...] * ok_other[...]
    else:
        ok_ref[...] = jnp.ones_like(ok_ref)
    to_near.wait_send()
    for copy in sel_send + link + forward + pass_near + back + again:
        copy.wait_send()


def solution(mesh):
    def layer(xcap, rcap, checked, collective_id, sel, gate, x_loc, up_loc, down_loc):
        tok, width = x_loc.shape
        experts, _, hidden = up_loc.shape
        vmem = pl.BlockSpec(memory_space=pltpu.VMEM)
        hbm = pl.BlockSpec(memory_space=pl.ANY)
        dma = pltpu.SemaphoreType.DMA
        entries = GROUPS * LANES
        four = dma((GROUPS,))
        return pl.pallas_call(
            functools.partial(moe_kernel, xcap, rcap, checked),
            out_shape=(jax.ShapeDtypeStruct((tok, width), BF16), jax.ShapeDtypeStruct((8, LANES), F32)),
            in_specs=[vmem, vmem, hbm, hbm, hbm],
            out_specs=(vmem, vmem),
            scratch_shapes=[
                pltpu.VMEM((2 * tok, width), BF16),
                pltpu.VMEM((sum(xcap) // 2, width), BF16),
                pltpu.VMEM((sum(xcap), width), BF16),
                pltpu.VMEM((entries, width), BF16),
                pltpu.VMEM((entries, width), BF16),
                pltpu.VMEM((entries, width), BF16),
                pltpu.VMEM((sum(rcap), width), BF16),
                pltpu.VMEM((2, sum(rcap), width), BF16),
                pltpu.VMEM((tok, width), F32),
                pltpu.VMEM((entries, 2 * tok), BF16),
                pltpu.VMEM((4, GROUPS, LANES), I32),
                pltpu.VMEM((4, GROUPS, LANES), I32),
                pltpu.VMEM((2, GROUPS, 1, LANES), I32),
                pltpu.VMEM((entries, 1), I32),
                pltpu.VMEM((entries, 1), F32),
                pltpu.VMEM((entries, 1), I32),
                pltpu.VMEM((8, LANES), I32),
                pltpu.VMEM((LANES, LANES), F32),
                pltpu.VMEM((8, LANES), F32),
                pltpu.VMEM((8, LANES), F32),
                pltpu.VMEM((RING, width, hidden), BF16),
                pltpu.VMEM((RING, hidden, width), BF16),
                dma, dma((RING,)), dma((RING,)), dma((3,)), dma((3,)), dma, dma,
                four, four, four, four, four, four, four, four, four, four, dma, dma,
            ],
            compiler_params=pltpu.CompilerParams(collective_id=collective_id, has_side_effects=True,
                                                 vmem_limit_bytes=64 * 1024 * 1024 - 65536),
        )(sel, gate, x_loc, up_loc, down_loc)

    def local_layer(x_loc, sel_loc, gate_loc, up_loc, down_loc):
        sel = sel_loc.reshape(GROUPS, LANES)
        gate = gate_loc.reshape(GROUPS, LANES)
        args = (sel, gate, x_loc, up_loc, down_loc)
        y, ok = layer((224, 128, 96, 96), (96, 96, 96, 128), True, 0, *args)
        return lax.cond(ok[0, 0] > 0.5, lambda: y, lambda: layer((256,) * 4, (128,) * 4, False, 1, *args)[0])

    row_spec = P(("dp", "ep"), None)
    weight_spec = P("ep", None, None)
    return jax.shard_map(local_layer, mesh=mesh, in_specs=(row_spec, row_spec, row_spec, weight_spec, weight_spec), out_specs=row_spec, check_vma=False)
```

```python
import functools

import jax
import jax.numpy as jnp
from jax import lax
from jax.experimental import pallas as pl
from jax.experimental.pallas import tpu as pltpu
from jax.sharding import PartitionSpec as P

MESH = pl.DeviceIdType.MESH
RING = 3
GROUPS = 4
LANES = 128
BF16 = jnp.bfloat16
F32 = jnp.float32
I32 = jnp.int32


def iota(shape, dim):
    return lax.broadcasted_iota(I32, shape, dim)


def mm(a, b):
    return jnp.dot(a.astype(BF16), b.astype(BF16), preferred_element_type=F32)


def mm_t(a, b):
    return lax.dot_general(a.astype(BF16), b.astype(BF16), (((1,), (1,)), ((), ())), preferred_element_type=F32)


def flag(cond):
    return jnp.where(cond, 1.0, 0.0)


def total(a):
    return jnp.sum(jnp.sum(a, axis=1, keepdims=True), axis=0, keepdims=True)


def moe_kernel(xcap, rcap, checked, sel_in, gate_in, x_hbm, up_hbm, down_hbm, y_ref, ok_ref,
               x_chip, x_out, x_in, picked, contrib, contrib_near, ret_out, ret_in, acc, hot,
               sels, slots, toks, sel_col, gate_col, need_col, pos_out, square, ok_mine, ok_other, up_buf, down_buf,
               x_sem, up_sem, down_sem, send_sel, recv_sel, send_x, recv_x, send_link, recv_link, send_fwd, recv_fwd,
               send_near, recv_near, send_ret, recv_ret, send_back, recv_back, send_ok, recv_ok):
    tok, width = y_ref.shape
    cap = 32
    experts = GROUPS * LANES // cap
    per_group = experts // GROUPS
    xoff = [sum(xcap[:i]) for i in range(GROUPS + 1)]
    roff = [sum(rcap[:i]) for i in range(GROUPS + 1)]
    me = lax.axis_index("ep")
    core = me % 2
    chip = me // 2
    near = me + 1 - 2 * core
    far = (me + 2) % 4
    diag = 3 - me
    peers = (near, far, diag)
    other_group = 1 - lax.axis_index("dp")

    def up_copy(e):
        return pltpu.make_async_copy(up_hbm.at[e], up_buf.at[e % RING], up_sem.at[e % RING])

    def down_copy(e):
        return pltpu.make_async_copy(down_hbm.at[e], down_buf.at[e % RING], down_sem.at[e % RING])

    def remote(src, dst, send, recv, peer, axis="ep"):
        return pltpu.make_async_remote_copy(src_ref=src, dst_ref=dst, send_sem=send, recv_sem=recv,
                                            device_id={axis: peer}, device_id_type=MESH)

    own_rows = pl.ds(pl.multiple_of(core * tok, tok), tok)
    near_rows = pl.ds(pl.multiple_of((1 - core) * tok, tok), tok)
    load_x = pltpu.make_async_copy(x_hbm, x_chip.at[own_rows], x_sem)
    load_x.start()

    barrier = pltpu.get_barrier_semaphore()
    for peer in peers:
        pl.semaphore_signal(barrier, inc=1, device_id={"ep": peer}, device_id_type=MESH)
    if checked:
        pl.semaphore_signal(barrier, inc=1, device_id={"dp": other_group}, device_id_type=MESH)
    for e in range(RING):
        up_copy(e).start()
        down_copy(e).start()
    pl.semaphore_wait(barrier, 4 if checked else 3)

    sel_send = [remote(sel_in, sels.at[me], send_sel.at[i], recv_sel.at[i], peer) for i, peer in enumerate(peers)]
    for copy in sel_send:
        copy.start()
    load_x.wait()
    to_near = remote(x_chip.at[own_rows], x_chip.at[own_rows], send_x, recv_x, near)
    to_near.start()
    sels[me] = sel_in[...]

    square[...] = jnp.zeros_like(square)
    square[0:GROUPS, :] = sel_in[...].astype(F32)
    square[8:8 + GROUPS, :] = gate_in[...]
    turned = square[...].T
    for j in range(GROUPS):
        sel_col[j * LANES:(j + 1) * LANES, :] = turned[:, j:j + 1].astype(I32)
        gate_col[j * LANES:(j + 1) * LANES, :] = turned[:, 8 + j:9 + j]
    for copy in sel_send:
        copy.wait_recv()

    before = flag(iota((LANES, LANES), 0) < iota((LANES, LANES), 1))
    ones = jnp.ones((LANES, LANES), F32)
    rows_before = flag(iota((GROUPS * 8, GROUPS * 8), 1) < iota((GROUPS * 8, GROUPS * 8), 0))

    def row_order(c):
        base = (1 - c) * (2 * tok)
        seen = jnp.zeros((8, LANES), F32)
        firsts, fits = [], []
        for j in range(GROUPS):
            row = jnp.concatenate([sels[2 * c, j:j + 1, :], sels[2 * c + 1, j:j + 1, :]], axis=1) - base
            high = flag(iota((8, 2 * LANES), 0) == (row >> 7))
            low = flag(iota((LANES, 2 * LANES), 0) == (row & 127))
            need = flag(mm_t(high, low) > 0.5)
            firsts.append(need * (1.0 - seen))
            seen = jnp.maximum(seen, need)
            fits.append(flag(total(seen) < xoff[j + 1] + 0.5))
        first = jnp.concatenate(firsts, axis=0)
        place = mm(first, before) + mm(rows_before, mm(first, ones))
        pos = sum(firsts[j] * (place[8 * j:8 * j + 8] + 1.0) for j in range(GROUPS)) - 1.0
        return pos, fits[0] * fits[1] * fits[2] * fits[3]

    def entry_order(d):
        away = flag((sels[d] >> 10) != d // 2)
        rank = mm(away, before)
        count = jnp.sum(away, axis=1, keepdims=True)
        end = jnp.zeros((1, 1), F32)
        for j in range(GROUPS):
            begin = jnp.maximum(end, float(roff[j]))
            slots[d, j:j + 1, :] = (away[j:j + 1] * (rank[j:j + 1] + begin + 1.0) - 1.0).astype(I32)
            end = begin + count[j:j + 1]
        return flag(end < roff[GROUPS] + 0.5)

    to_send, fit = row_order(1 - chip)
    pos_out[...] = to_send.astype(I32)
    to_near.wait_recv()

    link = []
    for i in range(GROUPS):
        part = xcap[i] // 2
        start = xoff[i] + core * part
        for b in range(8):
            hot[0:part, b * LANES:(b + 1) * LANES] = flag(iota((part, LANES), 0) + start == pos_out[b:b + 1, :]).astype(BF16)
        at = pl.ds(xoff[i] // 2, part)

        x_out[at, :] = jnp.dot(hot[0:part, 0:2 * tok], x_chip[:, :], preferred_element_type=F32).astype(BF16)

        link.append(remote(x_out.at[at], x_in.at[pl.ds(pl.multiple_of(start, 16), part)], send_link.at[i], recv_link.at[i], far))
        link[i].start()

    wanted, fit_in = row_order(chip)
    fit = fit * fit_in
    for d in range(4):
        fit = fit * entry_order(d)

    found = jnp.zeros((GROUPS * LANES, LANES), F32)
    for b in range(8):
        base = (1 - chip) * (2 * tok) + b * LANES
        found = found + jnp.where(sel_col[...] == iota((GROUPS * LANES, LANES), 1) + base, wanted[b:b + 1, :] + 1.0, 0.0)
    need_col[...] = (jnp.sum(found, axis=1, keepdims=True) - 1.0).astype(I32)

    for b in range(8):
        base = chip * (2 * tok) + b * LANES
        hot[:, b * LANES:(b + 1) * LANES] = flag(sel_col[...] == iota((GROUPS * LANES, LANES), 1) + base).astype(BF16)

    picked[:, :] = jnp.dot(hot[:, 0:2 * tok], x_chip[:, :], preferred_element_type=F32).astype(BF16)

    for f, d in enumerate((far, diag)):
        row = sels[d]
        for j in range(GROUPS):
            sums = jnp.zeros((8, LANES), F32)
            for k in range(j + 1):
                chosen = flag(iota((LANES, LANES), 0) + roff[j] == slots[d, k:k + 1, :])
                at = iota((8, LANES), 0)
                value = jnp.where(at == 0, row[k:k + 1] >> 5, jnp.where(at == 1, row[k:k + 1] & 31, 1)).astype(F32)
                sums = sums + mm_t(value, chosen)
            token = jnp.where((sums[2:3] > 0.5) & (iota((1, LANES), 1) < rcap[j]), sums[0:1] * 32.0 + sums[1:2], -1.0)
            toks[f, j] = token.astype(I32)

    if checked:
        ok_mine[...] = jnp.broadcast_to(fit, ok_mine.shape)
        ok_send = remote(ok_mine, ok_other, send_ok, recv_ok, other_group, "dp")
        ok_send.start()

    acc[...] = x_chip[own_rows, :].astype(F32)

    forward = []
    for i in range(GROUPS):
        part = xcap[i] // 2
        block = x_in.at[pl.ds(pl.multiple_of(xoff[i] + core * part, 16), part)]
        forward.append(remote(block, block, send_fwd.at[i], recv_fwd.at[i], near))

    def arrive(i):
        link[i].wait_recv()
        forward[i].start()
        r0, size = i * LANES, xcap[i]
        hot[r0:, 0:size] = flag(need_col[r0:, :] == iota((GROUPS * LANES - r0, size), 1) + xoff[i]).astype(BF16)
        forward[i].wait_recv()

        picked[r0:, :] = picked[r0:, :] + jnp.dot(
            hot[r0:, 0:size], x_in[xoff[i]:xoff[i + 1], :], preferred_element_type=F32).astype(BF16)

    pass_near, back = [], []
    for j in range(GROUPS):
        block = pl.ds(j * LANES, LANES)
        pass_near.append(remote(contrib.at[block], contrib_near.at[block], send_near.at[j], recv_near.at[j], near))
        block = pl.ds(roff[j], rcap[j])
        back.append(remote(ret_out.at[block], ret_in.at[0, block], send_ret.at[j], recv_ret.at[j], far))

    def give(j):
        pass_near[j].start()
        depth = (j + 1) * LANES
        for k in range(j + 1):
            hot[0:rcap[j], k * LANES:(k + 1) * LANES] = flag(
                iota((rcap[j], LANES), 0) + roff[j] == slots[me, k:k + 1, :]).astype(BF16)

        ret_out[roff[j]:roff[j + 1], :] = jnp.dot(
            hot[0:rcap[j], 0:depth], contrib[0:depth, :], preferred_element_type=F32).astype(BF16)

        back[j].start()

    def expert(e, carry):
        for i in range(GROUPS):
            pl.when(e == i * per_group)(functools.partial(arrive, i))
        rows = pl.ds(pl.multiple_of(e * cap, cap), cap)
        up_copy(e).wait()
        z = jnp.dot(picked[rows, :], up_buf[e % RING], preferred_element_type=F32)
        act = (0.5 * z * (1.0 + jnp.tanh(0.7978845608028654 * (z + 0.044715 * (z * z * z))))).astype(BF16)

        @pl.when(e + RING < experts)
        def _():
            up_copy(e + RING).start()

        down_copy(e).wait()
        for n in range(width // 512):
            cols = slice(n * 512, (n + 1) * 512)
            o = jnp.dot(act, down_buf[e % RING, :, cols], preferred_element_type=F32)
            contrib[rows, cols] = (o * gate_col[rows, :]).astype(BF16)

        @pl.when(e + RING < experts)
        def _():
            down_copy(e + RING).start()

        for j in range(GROUPS):
            pl.when(e == j * per_group + per_group - 1)(functools.partial(give, j))
        return carry

    lax.fori_loop(0, experts, expert, 0)

    def add_rows(d, source):
        for j in range(GROUPS):
            hot[:, j * LANES:(j + 1) * LANES] = flag(iota((tok, LANES), 0) + me * tok == sels[d, j:j + 1, :]).astype(BF16)

        acc[:, :] += jnp.dot(hot[:, 0:GROUPS * LANES], source[:, :], preferred_element_type=F32)

    def add_back(f, j):
        hot[:, 0:LANES] = flag(iota((tok, LANES), 0) + me * tok == toks[f, j]).astype(BF16)

        acc[:, :] += jnp.dot(hot[:, 0:rcap[j]], ret_in[f, roff[j]:roff[j + 1], :], preferred_element_type=F32)

    again = []
    for j in range(GROUPS):
        block = pl.ds(roff[j], rcap[j])
        again.append(remote(ret_in.at[0, block], ret_in.at[1, block], send_back.at[j], recv_back.at[j], near))

    add_rows(me, contrib)
    for j in range(GROUPS):
        pass_near[j].wait_recv()
    add_rows(near, contrib_near)
    for j in range(GROUPS):
        back[j].wait_recv()
        again[j].start()
        add_back(0, j)
        again[j].wait_recv()
        add_back(1, j)
    y_ref[...] = acc[...].astype(BF16)

    if checked:
        ok_send.wait()
        ok_ref[...] = ok_mine[...] * ok_other[...]
    else:
        ok_ref[...] = jnp.ones_like(ok_ref)
    to_near.wait_send()
    for copy in sel_send + link + forward + pass_near + back + again:
        copy.wait_send()


def solution(mesh):
    def layer(xcap, rcap, checked, collective_id, sel, gate, x_loc, up_loc, down_loc):
        tok, width = x_loc.shape
        experts, _, hidden = up_loc.shape
        vmem = pl.BlockSpec(memory_space=pltpu.VMEM)
        hbm = pl.BlockSpec(memory_space=pl.ANY)
        dma = pltpu.SemaphoreType.DMA
        entries = GROUPS * LANES
        four = dma((GROUPS,))
        return pl.pallas_call(
            functools.partial(moe_kernel, xcap, rcap, checked),
            out_shape=(jax.ShapeDtypeStruct((tok, width), BF16), jax.ShapeDtypeStruct((8, LANES), F32)),
            in_specs=[vmem, vmem, hbm, hbm, hbm],
            out_specs=(vmem, vmem),
            scratch_shapes=[
                pltpu.VMEM((2 * tok, width), BF16),
                pltpu.VMEM((sum(xcap) // 2, width), BF16),
                pltpu.VMEM((sum(xcap), width), BF16),
                pltpu.VMEM((entries, width), BF16),
                pltpu.VMEM((entries, width), BF16),
                pltpu.VMEM((entries, width), BF16),
                pltpu.VMEM((sum(rcap), width), BF16),
                pltpu.VMEM((2, sum(rcap), width), BF16),
                pltpu.VMEM((tok, width), F32),
                pltpu.VMEM((entries, 2 * tok), BF16),
                pltpu.VMEM((4, GROUPS, LANES), I32),
                pltpu.VMEM((4, GROUPS, LANES), I32),
                pltpu.VMEM((2, GROUPS, 1, LANES), I32),
                pltpu.VMEM((entries, 1), I32),
                pltpu.VMEM((entries, 1), F32),
                pltpu.VMEM((entries, 1), I32),
                pltpu.VMEM((8, LANES), I32),
                pltpu.VMEM((LANES, LANES), F32),
                pltpu.VMEM((8, LANES), F32),
                pltpu.VMEM((8, LANES), F32),
                pltpu.VMEM((RING, width, hidden), BF16),
                pltpu.VMEM((RING, hidden, width), BF16),
                dma, dma((RING,)), dma((RING,)), dma((3,)), dma((3,)), dma, dma,
                four, four, four, four, four, four, four, four, four, four, dma, dma,
            ],
            compiler_params=pltpu.CompilerParams(collective_id=collective_id, has_side_effects=True,
                                                 vmem_limit_bytes=64 * 1024 * 1024 - 65536),
        )(sel, gate, x_loc, up_loc, down_loc)

    def local_layer(x_loc, sel_loc, gate_loc, up_loc, down_loc):
        sel = sel_loc.reshape(GROUPS, LANES)
        gate = gate_loc.reshape(GROUPS, LANES)
        args = (sel, gate, x_loc, up_loc, down_loc)
        y, ok = layer((224, 128, 96, 96), (96, 96, 96, 128), True, 0, *args)
        return lax.cond(ok[0, 0] > 0.5, lambda: y, lambda: layer((256,) * 4, (128,) * 4, False, 1, *args)[0])

    row_spec = P(("dp", "ep"), None)
    weight_spec = P("ep", None, None)
    return jax.shard_map(local_layer, mesh=mesh, in_specs=(row_spec, row_spec, row_spec, weight_spec, weight_spec), out_specs=row_spec, check_vma=False)
```

```python
import functools

import jax
import jax.numpy as jnp
from jax import lax
from jax.experimental import pallas as pl
from jax.experimental.pallas import tpu as pltpu
from jax.sharding import PartitionSpec as P

MESH = pl.DeviceIdType.MESH
GROUPS = 4
LANES = 128
ENTRIES = GROUPS * LANES
BF16 = jnp.bfloat16
F32 = jnp.float32
I32 = jnp.int32
SENT_AFTER = (None, None, 3, 7, 11, 13, 15)
CHUNKS = len(SENT_AFTER)
FIT = dict(sizes=(112, 64, 80, 96, 96, 48, 80), ring=3, step=2048, checked=True)
FULL = dict(sizes=(128, 128, 256, 256, 128, 64, 64), ring=2, step=512, checked=False)


def iota(shape, dim):
    return lax.broadcasted_iota(I32, shape, dim)


def mm(a, b):
    return jnp.dot(a.astype(BF16), b.astype(BF16), preferred_element_type=F32)


def mm_t(a, b):
    return lax.dot_general(a.astype(BF16), b.astype(BF16), (((1,), (1,)), ((), ())), preferred_element_type=F32)


def flag(cond):
    return jnp.where(cond, 1.0, 0.0)


def total(a):
    return jnp.sum(jnp.sum(a, axis=1, keepdims=True), axis=0, keepdims=True)


def plan(sizes):
    off = [sum(sizes[:c]) for c in range(CHUNKS + 1)]
    base = [2 * off[c] + (2 * ENTRIES if c >= 2 else 0) for c in range(CHUNKS + 1)]
    return off, base, 2 * off[2], 2 * off[2] + ENTRIES


def moe_kernel(sizes, ring, step, checked, sel_in, gate_in, x_hbm, up_hbm, down_hbm, y_ref, ok_ref,
               x_chip, out, rows_in, picked, acc, hot,
               sel_row, sels, slots, toks_a, toks_b, sel_col, gate_col, need_col, pos_out, square, ok_mine, ok_other,
               up_buf, down_buf,
               x_sem, up_sem, down_sem, send_sel, recv_sel, send_x, recv_x, send_link, recv_link, send_fwd, recv_fwd,
               send_near, recv_near, send_ok, recv_ok):
    tok, width = y_ref.shape
    experts, cap = sel_in.shape
    per_group = experts // GROUPS
    off, base, own_at, near_at = plan(sizes)
    me = lax.axis_index("ep")
    core = me % 2
    chip = me // 2
    near = me + 1 - 2 * core
    far = (me + 2) % 4
    diag = 3 - me
    peers = (near, far, diag)
    other_group = 1 - lax.axis_index("dp")

    def up_copy(e):
        return pltpu.make_async_copy(up_hbm.at[e], up_buf.at[e % ring], up_sem.at[e % ring])

    def down_copy(e):
        return pltpu.make_async_copy(down_hbm.at[e], down_buf.at[e % ring], down_sem.at[e % ring])

    def remote(src, dst, send, recv, peer, axis="ep"):
        return pltpu.make_async_remote_copy(src_ref=src, dst_ref=dst, send_sem=send, recv_sem=recv,
                                            device_id={axis: peer}, device_id_type=MESH)

    def by_columns(write):
        if step == width:
            write(slice(None))
        else:
            @pl.loop(0, width // step)
            def _(n):
                write(pl.ds(pl.multiple_of(n * step, step), step))

    own_rows = pl.ds(pl.multiple_of(core * tok, tok), tok)
    load_x = pltpu.make_async_copy(x_hbm, x_chip.at[own_rows], x_sem)
    load_x.start()

    barrier = pltpu.get_barrier_semaphore()
    for peer in peers:
        pl.semaphore_signal(barrier, inc=1, device_id={"ep": peer}, device_id_type=MESH)
    if checked:
        pl.semaphore_signal(barrier, inc=1, device_id={"dp": other_group}, device_id_type=MESH)
    for e in range(ring):
        up_copy(e).start()
        down_copy(e).start()

    spread = flag(iota((cap, LANES), 0) == iota((cap, LANES), 1) % cap)
    inside = flag(iota((experts, LANES), 0) % per_group == iota((experts, LANES), 1) // cap)
    gather = flag(iota((GROUPS, experts), 1) // per_group == iota((GROUPS, experts), 0))
    high = mm(gather, mm((sel_in[...] >> 5).astype(F32), spread) * inside)
    low = mm(gather, mm((sel_in[...] & 31).astype(F32), spread) * inside)
    sel_row[...] = (high * 32.0 + low).astype(I32)
    square[...] = jnp.zeros_like(square)
    square[0:experts, 0:cap] = sel_in[...].astype(F32)
    square[experts:2 * experts, 0:cap] = gate_in[...]
    turned = square[...].T
    for e in range(experts):
        sel_col[e * cap:(e + 1) * cap, :] = turned[0:cap, e:e + 1].astype(I32)
        gate_col[e * cap:(e + 1) * cap, :] = turned[0:cap, experts + e:experts + e + 1]

    pl.semaphore_wait(barrier, 4 if checked else 3)
    sel_send = [remote(sel_row, sels.at[me], send_sel.at[i], recv_sel.at[i], peer) for i, peer in enumerate(peers)]
    for copy in sel_send:
        copy.start()
    load_x.wait()
    to_near = remote(x_chip.at[own_rows], x_chip.at[own_rows], send_x, recv_x, near)
    to_near.start()
    sels[me] = sel_row[...]

    before = flag(iota((LANES, LANES), 0) < iota((LANES, LANES), 1))
    ones = jnp.ones((LANES, LANES), F32)
    rows_before = flag(iota((GROUPS * 8, GROUPS * 8), 1) < iota((GROUPS * 8, GROUPS * 8), 0))
    for copy in sel_send:
        copy.wait_recv()

    def row_order(c):
        start = (1 - c) * (2 * tok)
        seen = jnp.zeros((8, LANES), F32)
        firsts, fit = [], jnp.ones((1, 1), F32)
        for j in range(GROUPS):
            row = jnp.concatenate([sels[2 * c, j:j + 1, :], sels[2 * c + 1, j:j + 1, :]], axis=1) - start
            row_high = flag(iota((8, 2 * LANES), 0) == (row >> 7))
            row_low = flag(iota((LANES, 2 * LANES), 0) == (row & 127))
            need = flag(mm_t(row_high, row_low) > 0.5)
            firsts.append(need * (1.0 - seen))
            seen = jnp.maximum(seen, need)
            fit = fit * flag(total(seen) < 2.0 * off[j + 1] + 0.5)
        first = jnp.concatenate(firsts, axis=0)
        place = mm(first, before) + mm(rows_before, mm(first, ones))
        pos = sum(firsts[j] * (place[8 * j:8 * j + 8] + 1.0) for j in range(GROUPS)) - 1.0
        return pos.astype(I32), total(seen), fit

    def entry_order(d, sent_rows):
        away = flag((sels[d] >> 10) != d // 2)
        rank = mm(away, before)
        lane = iota((GROUPS, LANES), 1)
        early = flag(lane < LANES // 2)
        count = jnp.sum(away, axis=1, keepdims=True)
        count_early = jnp.sum(away * early, axis=1, keepdims=True)
        end = jnp.floor((sent_rows + 1.0) * 0.5)
        for j in range(GROUPS):
            row = slice(j, j + 1)
            begin = jnp.maximum(end, float(off[j + 2]))
            place = rank[row] + begin
            end = begin + count[row]
            if j == GROUPS - 1:
                later = jnp.maximum(begin + count_early[row], float(off[CHUNKS - 1]))
                place = jnp.where(lane[row] < LANES // 2, place, rank[row] - count_early[row] + later)
                end = later + count[row] - count_early[row]
            slots[d, row, :] = (away[row] * (place + 1.0) - 1.0).astype(I32)
        return flag(end < off[CHUNKS] + 0.5)

    pos, rows_sent, fit = row_order(1 - chip)
    pos_out[...] = jnp.where((pos & 1) == core, pos >> 1, -1)
    to_near.wait_recv()

    def pack(lo, hi):
        size = off[hi] - off[lo]
        for b in range(8):
            hot[0:size, b * LANES:(b + 1) * LANES] = flag(iota((size, LANES), 0) + off[lo] == pos_out[b:b + 1, :]).astype(BF16)

        def write(cols):
            out[off[lo]:off[hi], cols] = jnp.dot(hot[0:size, 0:2 * tok], x_chip[:, cols],
                                                 preferred_element_type=F32).astype(BF16)
        by_columns(write)

    link, forward = [], []
    for c in range(CHUNKS):
        mine = rows_in.at[pl.ds(base[c], sizes[c])]
        theirs = rows_in.at[pl.ds(base[c] + sizes[c], sizes[c])]
        link.append(remote(out.at[pl.ds(off[c], sizes[c])], mine, send_link.at[c], recv_link.at[c], far))
        forward.append(remote(mine, theirs, send_fwd.at[c], recv_fwd.at[c], near))
    pass_near = []
    for j in range(GROUPS):
        pass_near.append(remote(rows_in.at[pl.ds(own_at + j * LANES, LANES)], rows_in.at[pl.ds(near_at + j * LANES, LANES)],
                                send_near.at[j], recv_near.at[j], near))

    pack(0, 2)
    link[0].start()
    link[1].start()
    pack(2, 4)

    wanted, rows_got, fit_in = row_order(chip)
    fit = fit * fit_in
    for d in range(4):
        same_chip = flag(jnp.full((1, 1), d // 2, I32) == chip)
        fit = fit * entry_order(d, same_chip * rows_sent + (1.0 - same_chip) * rows_got)

    slot = wanted >> 1
    side = jnp.where((wanted & 1) == core, 0, 1)
    where_in = jnp.full((8, LANES), -1, I32)
    for c in range(GROUPS):
        here = (slot >= off[c]) & (slot < off[c + 1]) & (wanted >= 0)
        where_in = jnp.where(here, base[c] - off[c] + slot + side * sizes[c], where_in)
    where_in = where_in.astype(F32)
    found = jnp.zeros((ENTRIES, LANES), F32)
    for b in range(8):
        start = (1 - chip) * (2 * tok) + b * LANES
        found = found + jnp.where(sel_col[...] == iota((ENTRIES, LANES), 1) + start, where_in[b:b + 1, :] + 1.0, 0.0)
    need_col[...] = (jnp.sum(found, axis=1, keepdims=True) - 1.0).astype(I32)

    for b in range(8):
        start = chip * (2 * tok) + b * LANES
        hot[0:ENTRIES, b * LANES:(b + 1) * LANES] = flag(sel_col[...] == iota((ENTRIES, LANES), 1) + start).astype(BF16)

    def pick_local(cols):
        picked[:, cols] = jnp.dot(hot[0:ENTRIES, 0:2 * tok], x_chip[:, cols], preferred_element_type=F32).astype(BF16)
    by_columns(pick_local)

    values = []
    for d in (far, diag):
        for k in range(GROUPS):
            at = iota((8, LANES), 0)
            row = sels[d, k:k + 1, :]
            values.append(jnp.where(at == 0, row >> 5, jnp.where(at == 1, row & 31, 1)).astype(F32))
    values = jnp.concatenate(values, axis=1)
    for c in range(2, CHUNKS):
        size = sizes[c]
        at = iota((2 * size, LANES), 0)
        for f, d in enumerate((far, diag)):
            key = jnp.where((at >= f * size) & (at < (f + 1) * size), at - f * size + off[c], -2)
            for k in range(GROUPS):
                block = (f * GROUPS + k) * LANES
                hot[0:2 * size, block:block + LANES] = flag(key == slots[d, k:k + 1, :]).astype(BF16)
        sums = mm_t(values, hot[0:2 * size, 0:2 * ENTRIES])
        token = jnp.where(sums[2:3] > 0.5, sums[0:1] * 32.0 + sums[1:2], -1.0).astype(I32)
        if c < 5:
            toks_a[:, base[c] - base[2]:base[c + 1] - base[2]] = token
        else:
            toks_b[:, base[c] - base[5]:base[c + 1] - base[5]] = token

    if checked:
        ok_mine[...] = jnp.broadcast_to(fit, ok_mine.shape)
        ok_send = remote(ok_mine, ok_other, send_ok, recv_ok, other_group, "dp")
        ok_send.start()

    def arrive(c):
        link[c].wait_recv()
        forward[c].start()
        r0, size = c * LANES, 2 * sizes[c]
        hot[r0:ENTRIES, 0:size] = flag(need_col[r0:, :] == iota((ENTRIES - r0, size), 1) + base[c]).astype(BF16)
        forward[c].wait_recv()

        def write(cols):
            picked[r0:, cols] = picked[r0:, cols] + jnp.dot(
                hot[r0:ENTRIES, 0:size], rows_in[base[c]:base[c] + size, cols], preferred_element_type=F32).astype(BF16)
        by_columns(write)

    def give(c):
        size = sizes[c]
        depth = (SENT_AFTER[c] + 1) * cap
        for k in range(0, depth, LANES):
            part = min(LANES, depth - k)
            row = slots[me, k // LANES:k // LANES + 1, 0:part]
            hot[0:size, k:k + part] = flag(iota((size, part), 0) + off[c] == row).astype(BF16)

        def write(cols):
            packed = jnp.dot(hot[0:size, 0:depth], rows_in[own_at:own_at + depth, cols],
                             preferred_element_type=F32).astype(BF16)
            if c < GROUPS:
                packed = packed + out[off[c]:off[c + 1], cols]
            out[off[c]:off[c + 1], cols] = packed
        by_columns(write)
        link[c].start()

    def expert(e, carry):
        for c in range(GROUPS):
            pl.when(e == c * per_group)(functools.partial(arrive, c))
        rows = pl.ds(pl.multiple_of(e * cap, cap), cap)
        own = pl.ds(pl.multiple_of(own_at + e * cap, 32), cap)
        up_copy(e).wait()
        z = jnp.dot(picked[rows, :], up_buf[e % ring], preferred_element_type=F32)
        act = (0.5 * z * (1.0 + jnp.tanh(0.7978845608028654 * (z + 0.044715 * (z * z * z))))).astype(BF16)

        @pl.when(e + ring < experts)
        def _():
            up_copy(e + ring).start()

        down_copy(e).wait()
        for n in range(width // 512):
            cols = slice(n * 512, (n + 1) * 512)
            o = jnp.dot(act, down_buf[e % ring, :, cols], preferred_element_type=F32)
            rows_in[own, cols] = (o * gate_col[rows, :]).astype(BF16)

        @pl.when(e + ring < experts)
        def _():
            down_copy(e + ring).start()

        for c in range(2, CHUNKS):
            pl.when(e == SENT_AFTER[c])(functools.partial(give, c))
        for j in range(GROUPS):
            pl.when(e == j * per_group + per_group - 1)(pass_near[j].start)
        return carry

    lax.fori_loop(0, experts, expert, 0)

    link[4].wait_recv()
    forward[4].start()
    early = base[5] - own_at
    for at, d in ((0, me), (ENTRIES, near)):
        for k in range(GROUPS):
            hot[0:tok, at + k * LANES:at + (k + 1) * LANES] = flag(
                iota((tok, LANES), 0) + me * tok == sels[d, k:k + 1, :]).astype(BF16)
    hot[0:tok, 2 * ENTRIES:early] = flag(iota((tok, early - 2 * ENTRIES), 0) + me * tok == toks_a[...]).astype(BF16)
    for copy in pass_near:
        copy.wait_recv()
    forward[4].wait_recv()

    def add_early(cols):
        acc[:, cols] = x_chip[own_rows, cols].astype(F32) + jnp.dot(
            hot[0:tok, 0:early], rows_in[own_at:base[5], cols], preferred_element_type=F32)
    by_columns(add_early)

    late = base[CHUNKS] - base[5]
    for c in (5, 6):
        link[c].wait_recv()
        forward[c].start()
    hot[0:tok, 0:late] = flag(iota((tok, late), 0) + me * tok == toks_b[...]).astype(BF16)
    for c in (5, 6):
        forward[c].wait_recv()

    def add_late(cols):
        y_ref[:, cols] = (acc[:, cols] + jnp.dot(hot[0:tok, 0:late], rows_in[base[5]:base[CHUNKS], cols],
                                                 preferred_element_type=F32)).astype(BF16)
    by_columns(add_late)

    if checked:
        ok_send.wait()
        ok_ref[0, 0] = jnp.min(ok_mine[...] * ok_other[...])
    else:
        ok_ref[0, 0] = 1.0
    to_near.wait_send()
    for copy in sel_send + link + forward + pass_near:
        copy.wait_send()


def solution(mesh):
    def layer(sizes, ring, step, checked, collective_id, sel, gate, x_loc, up_loc, down_loc):
        tok, width = x_loc.shape
        experts, _, hidden = up_loc.shape
        off, base, own_at, _ = plan(sizes)
        vmem = pl.BlockSpec(memory_space=pltpu.VMEM)
        hbm = pl.BlockSpec(memory_space=pl.ANY)
        dma = pltpu.SemaphoreType.DMA
        each = dma((CHUNKS,))
        return pl.pallas_call(
            functools.partial(moe_kernel, sizes, ring, step, checked),
            out_shape=(jax.ShapeDtypeStruct((tok, width), BF16), jax.ShapeDtypeStruct((1, 1), F32)),
            in_specs=[vmem, vmem, hbm, hbm, hbm],
            out_specs=(vmem, pl.BlockSpec(memory_space=pltpu.SMEM)),
            scratch_shapes=[
                pltpu.VMEM((2 * tok, width), BF16),
                pltpu.VMEM((off[CHUNKS], width), BF16),
                pltpu.VMEM((base[CHUNKS], width), BF16),
                pltpu.VMEM((ENTRIES, width), BF16),
                pltpu.VMEM((tok, width), F32),
                pltpu.VMEM((tok, max(2 * tok, base[5] - own_at)), BF16),
                pltpu.VMEM((GROUPS, LANES), I32),
                pltpu.VMEM((4, GROUPS, LANES), I32),
                pltpu.VMEM((4, GROUPS, LANES), I32),
                pltpu.VMEM((1, base[5] - base[2]), I32),
                pltpu.VMEM((1, base[CHUNKS] - base[5]), I32),
                pltpu.VMEM((ENTRIES, 1), I32),
                pltpu.VMEM((ENTRIES, 1), F32),
                pltpu.VMEM((ENTRIES, 1), I32),
                pltpu.VMEM((8, LANES), I32),
                pltpu.VMEM((LANES, LANES), F32),
                pltpu.VMEM((8, LANES), F32),
                pltpu.VMEM((8, LANES), F32),
                pltpu.VMEM((ring, width, hidden), BF16),
                pltpu.VMEM((ring, hidden, width), BF16),
                dma, dma((ring,)), dma((ring,)), dma((3,)), dma((3,)), dma, dma,
                each, each, each, each, dma((GROUPS,)), dma((GROUPS,)), dma, dma,
            ],
            compiler_params=pltpu.CompilerParams(collective_id=collective_id, has_side_effects=True,
                                                 vmem_limit_bytes=64 * 1024 * 1024 - 65536),
        )(sel, gate, x_loc, up_loc, down_loc)

    def local_layer(x_loc, sel_loc, gate_loc, up_loc, down_loc):
        args = (sel_loc, gate_loc, x_loc, up_loc, down_loc)
        y, ok = layer(*FIT.values(), 0, *args)
        return lax.cond(ok[0, 0] > 0.5, lambda: y, lambda: layer(*FULL.values(), 1, *args)[0])

    row_spec = P(("dp", "ep"), None)
    weight_spec = P("ep", None, None)
    return jax.shard_map(local_layer, mesh=mesh, in_specs=(row_spec, row_spec, row_spec, weight_spec, weight_spec), out_specs=row_spec, check_vma=False)
```

```python
import functools

import jax
import jax.numpy as jnp
from jax import lax
from jax.experimental import pallas as pl
from jax.experimental.pallas import tpu as pltpu
from jax.sharding import PartitionSpec as P

MESH = pl.DeviceIdType.MESH
GROUPS = 4
LANES = 128
ENTRIES = GROUPS * LANES
BF16 = jnp.bfloat16
F32 = jnp.float32
I32 = jnp.int32
SENT_AFTER = (None, None, None, None, 1, 3, 5, 7, 9, 11, 13, 15)
CHUNKS = len(SENT_AFTER)
FIRST = 4
X_FROM = (0, 2, 4, 6, 8, 12, 16)
X_LAST = (0, 1, 2, 3, 4, 6)
XGROUPS = len(X_LAST)
XCHUNKS = X_LAST[-1] + 1
LATE = CHUNKS - 2
FIT = dict(sizes=(64, 48, 32, 32, 48, 32, 48, 48, 48, 48, 64, 64), ring=3, step=2048, checked=True)
FULL = dict(sizes=(64, 64, 64, 64, 128, 64, 64, 192, 128, 64, 64, 64), ring=2, step=512, checked=False)


def iota(shape, dim):
    return lax.broadcasted_iota(I32, shape, dim)


def mm(a, b):
    return jnp.dot(a.astype(BF16), b.astype(BF16), preferred_element_type=F32)


def mm_t(a, b):
    return lax.dot_general(a.astype(BF16), b.astype(BF16), (((1,), (1,)), ((), ())), preferred_element_type=F32)


def flag(cond):
    return jnp.where(cond, 1.0, 0.0)


def total(a):
    return jnp.sum(jnp.sum(a, axis=1, keepdims=True), axis=0, keepdims=True)


def plan(sizes):
    off = [sum(sizes[:c]) for c in range(CHUNKS + 1)]
    near_at = [2 * off[FIRST] + j * LANES for j in range(GROUPS - 1)]
    shift = (GROUPS - 1) * LANES
    own_at = 2 * off[XCHUNKS] + shift
    near_at.append(own_at + ENTRIES)
    base = [2 * off[c] + (0 if c < FIRST else shift if c < XCHUNKS else shift + ENTRIES + LANES) for c in range(CHUNKS + 1)]
    return off, base, own_at, near_at


def lanes(n):
    return -(-n // LANES) * LANES


def moe_kernel(sizes, ring, step, checked, sel_in, gate_in, x_hbm, up_hbm, down_hbm, y_ref, ok_ref,
               x_chip, out, rows_in, picked, acc, hot,
               sel_row, sels, slots, toks_a, toks_b, toks_c, sel_col, gate_col, need_col, pos_out, square, ok_mine, ok_other,
               up_buf, down_buf,
               x_sem, up_sem, down_sem, send_sel, recv_sel, send_x, recv_x, send_link, recv_link, send_fwd, recv_fwd,
               send_near, recv_near, send_ok, recv_ok):
    tok, width = y_ref.shape
    experts, cap = sel_in.shape
    per_group = experts // GROUPS
    off, base, own_at, near_at = plan(sizes)
    me = lax.axis_index("ep")
    core = me % 2
    chip = me // 2
    near = me + 1 - 2 * core
    far = (me + 2) % 4
    diag = 3 - me
    peers = (near, far, diag)
    other_group = 1 - lax.axis_index("dp")

    def up_copy(e):
        return pltpu.make_async_copy(up_hbm.at[e], up_buf.at[e % ring], up_sem.at[e % ring])

    def down_copy(e):
        return pltpu.make_async_copy(down_hbm.at[e], down_buf.at[e % ring], down_sem.at[e % ring])

    def remote(src, dst, send, recv, peer, axis="ep"):
        return pltpu.make_async_remote_copy(src_ref=src, dst_ref=dst, send_sem=send, recv_sem=recv,
                                            device_id={axis: peer}, device_id_type=MESH)

    def by_columns(write):
        if step == width:
            write(slice(None))
        else:
            @pl.loop(0, width // step)
            def _(n):
                write(pl.ds(pl.multiple_of(n * step, step), step))

    own_rows = pl.ds(pl.multiple_of(core * tok, tok), tok)
    load_x = pltpu.make_async_copy(x_hbm, x_chip.at[own_rows], x_sem)
    load_x.start()

    barrier = pltpu.get_barrier_semaphore()
    for peer in peers:
        pl.semaphore_signal(barrier, inc=1, device_id={"ep": peer}, device_id_type=MESH)
    if checked:
        pl.semaphore_signal(barrier, inc=1, device_id={"dp": other_group}, device_id_type=MESH)
    for e in range(ring):
        up_copy(e).start()
        down_copy(e).start()

    spread = flag(iota((cap, LANES), 0) == iota((cap, LANES), 1) % cap)
    inside = flag(iota((experts, LANES), 0) % per_group == iota((experts, LANES), 1) // cap)
    gather = flag(iota((GROUPS, experts), 1) // per_group == iota((GROUPS, experts), 0))
    high = mm(gather, mm((sel_in[...] >> 5).astype(F32), spread) * inside)
    low = mm(gather, mm((sel_in[...] & 31).astype(F32), spread) * inside)
    sel_row[...] = (high * 32.0 + low).astype(I32)
    pl.semaphore_wait(barrier, 4 if checked else 3)
    sel_send = [remote(sel_row, sels.at[me], send_sel.at[i], recv_sel.at[i], peer) for i, peer in enumerate(peers)]
    for copy in sel_send:
        copy.start()
    load_x.wait()
    to_near = remote(x_chip.at[own_rows], x_chip.at[own_rows], send_x, recv_x, near)
    to_near.start()
    sels[me] = sel_row[...]
    square[...] = jnp.zeros_like(square)
    square[0:experts, 0:cap] = sel_in[...].astype(F32)
    square[experts:2 * experts, 0:cap] = gate_in[...]
    turned = square[...].T
    for e in range(experts):
        sel_col[e * cap:(e + 1) * cap, :] = turned[0:cap, e:e + 1].astype(I32)
        gate_col[e * cap:(e + 1) * cap, :] = turned[0:cap, experts + e:experts + e + 1]

    before = flag(iota((LANES, LANES), 0) < iota((LANES, LANES), 1))
    ones = jnp.ones((LANES, LANES), F32)
    rows_before = flag(iota((XGROUPS * 8, XGROUPS * 8), 1) < iota((XGROUPS * 8, XGROUPS * 8), 0))
    for copy in sel_send:
        copy.wait_recv()

    def row_order(c):
        start = (1 - c) * (2 * tok)
        seen = jnp.zeros((8, LANES), F32)
        firsts, fit = [], jnp.ones((1, 1), F32)
        lane = iota((1, 2 * LANES), 1) % LANES
        for j in range(XGROUPS):
            k = X_FROM[j] * cap // LANES
            row = jnp.concatenate([sels[2 * c, k:k + 1, :], sels[2 * c + 1, k:k + 1, :]], axis=1) - start
            if X_FROM[j + 1] - X_FROM[j] < per_group:
                from_lane = (X_FROM[j] % per_group) * cap
                row = jnp.where((lane >= from_lane) & (lane < from_lane + (X_FROM[j + 1] - X_FROM[j]) * cap), row, -1)
            row_high = flag(iota((8, 2 * LANES), 0) == (row >> 7))
            row_low = flag(iota((LANES, 2 * LANES), 0) == (row & 127))
            need = flag(mm_t(row_high, row_low) > 0.5)
            firsts.append(need * (1.0 - seen))
            seen = jnp.maximum(seen, need)
            fit = fit * flag(total(seen) < 2.0 * off[X_LAST[j] + 1] + 0.5)
        first = jnp.concatenate(firsts, axis=0)
        place = mm(first, before) + mm(rows_before, mm(first, ones))
        pos = sum(firsts[j] * (place[8 * j:8 * j + 8] + 1.0) for j in range(XGROUPS)) - 1.0
        return pos.astype(I32), total(seen), fit

    def entry_order(d, sent_rows):
        away = flag((sels[d] >> 10) != d // 2)
        rank = mm(away, before)
        lane = iota((GROUPS, LANES), 1)
        early = flag(lane < LANES // 2)
        count = jnp.sum(away, axis=1, keepdims=True)
        count_early = jnp.sum(away * early, axis=1, keepdims=True)
        end = jnp.floor((sent_rows + 1.0) * 0.5)
        for j in range(GROUPS):
            row = slice(j, j + 1)
            begin = jnp.maximum(end, float(off[FIRST + 2 * j]))
            later = jnp.maximum(begin + count_early[row], float(off[FIRST + 2 * j + 1]))
            place = rank[row] + jnp.where(lane[row] < LANES // 2, begin, later - count_early[row])
            end = later + count[row] - count_early[row]
            slots[d, row, :] = (away[row] * (place + 1.0) - 1.0).astype(I32)
        return flag(end < off[CHUNKS] + 0.5)

    pos, rows_sent, fit = row_order(1 - chip)
    pos_out[...] = jnp.where((pos & 1) == core, pos >> 1, -1)
    to_near.wait_recv()

    def pack(lo, hi):
        size = off[hi] - off[lo]
        for b in range(8):
            hot[0:size, b * LANES:(b + 1) * LANES] = flag(iota((size, LANES), 0) + off[lo] == pos_out[b:b + 1, :]).astype(BF16)

        def write(cols):
            out[off[lo]:off[hi], cols] = jnp.dot(hot[0:size, 0:2 * tok], x_chip[:, cols],
                                                 preferred_element_type=F32).astype(BF16)
        by_columns(write)

    link, forward = [], []
    for c in range(CHUNKS):
        mine = rows_in.at[pl.ds(base[c], sizes[c])]
        theirs = rows_in.at[pl.ds(base[c] + sizes[c], sizes[c])]
        link.append(remote(out.at[pl.ds(off[c], sizes[c])], mine, send_link.at[c], recv_link.at[c], far))
        forward.append(remote(mine, theirs, send_fwd.at[c], recv_fwd.at[c], near))
    pass_near = []
    for j in range(GROUPS):
        pass_near.append(remote(rows_in.at[pl.ds(own_at + j * LANES, LANES)], rows_in.at[pl.ds(near_at[j], LANES)],
                                send_near.at[j], recv_near.at[j], near))

    pack(0, FIRST)
    for c in range(FIRST):
        link[c].start()
    pack(FIRST, XCHUNKS)

    wanted, rows_got, fit_in = row_order(chip)
    fit = fit * fit_in
    for d in range(4):
        same_chip = flag(jnp.full((1, 1), d // 2, I32) == chip)
        fit = fit * entry_order(d, same_chip * rows_sent + (1.0 - same_chip) * rows_got)

    slot = wanted >> 1
    side = jnp.where((wanted & 1) == core, 0, 1)
    where_in = jnp.full((8, LANES), -1, I32)
    for c in range(XCHUNKS):
        here = (slot >= off[c]) & (slot < off[c + 1]) & (wanted >= 0)
        where_in = jnp.where(here, base[c] - off[c] + slot + side * sizes[c], where_in)
    where_in = where_in.astype(F32)
    found = jnp.zeros((ENTRIES, LANES), F32)
    for b in range(8):
        start = (1 - chip) * (2 * tok) + b * LANES
        found = found + jnp.where(sel_col[...] == iota((ENTRIES, LANES), 1) + start, where_in[b:b + 1, :] + 1.0, 0.0)
    need_col[...] = (jnp.sum(found, axis=1, keepdims=True) - 1.0).astype(I32)

    for b in range(8):
        start = chip * (2 * tok) + b * LANES
        hot[0:ENTRIES, b * LANES:(b + 1) * LANES] = flag(sel_col[...] == iota((ENTRIES, LANES), 1) + start).astype(BF16)

    def pick_local(cols):
        picked[:, cols] = jnp.dot(hot[0:ENTRIES, 0:2 * tok], x_chip[:, cols], preferred_element_type=F32).astype(BF16)
    by_columns(pick_local)

    values = []
    for d in (far, diag):
        for k in range(GROUPS):
            at = iota((8, LANES), 0)
            row = sels[d, k:k + 1, :]
            values.append(jnp.where(at == 0, row >> 5, jnp.where(at == 1, row & 31, 1)).astype(F32))
    values = jnp.concatenate(values, axis=1)
    for c in range(FIRST, CHUNKS):
        size = sizes[c]
        at = iota((2 * size, LANES), 0)
        for f, d in enumerate((far, diag)):
            key = jnp.where((at >= f * size) & (at < (f + 1) * size), at - f * size + off[c], -2)
            for k in range(GROUPS):
                block = (f * GROUPS + k) * LANES
                hot[0:2 * size, block:block + LANES] = flag(key == slots[d, k:k + 1, :]).astype(BF16)
        sums = mm_t(values, hot[0:2 * size, 0:2 * ENTRIES])
        token = jnp.where(sums[2:3] > 0.5, sums[0:1] * 32.0 + sums[1:2], -1.0).astype(I32)
        toks, start = (toks_a, FIRST) if c < XCHUNKS else (toks_b, XCHUNKS) if c < LATE else (toks_c, LATE)
        at = base[c] - base[start]
        toks[:, at:at + 2 * size] = token

    if checked:
        ok_mine[...] = jnp.broadcast_to(fit, ok_mine.shape)
        ok_send = remote(ok_mine, ok_other, send_ok, recv_ok, other_group, "dp")
        ok_send.start()

    def pass_on(c):
        link[c].wait_recv()
        forward[c].start()

    def arrive(j):
        r0, lo, hi = X_FROM[j] * cap, (X_LAST[j - 1] + 1 if j else 0), X_LAST[j] + 1
        size = base[hi - 1] + 2 * sizes[hi - 1] - base[lo]
        if j < 2:
            pass_on(lo)
        hot[r0:ENTRIES, 0:size] = flag(need_col[r0:, :] == iota((ENTRIES - r0, size), 1) + base[lo]).astype(BF16)
        for c in range(lo, hi):
            forward[c].wait_recv()

        def write(cols):
            picked[r0:, cols] = picked[r0:, cols] + jnp.dot(
                hot[r0:ENTRIES, 0:size], rows_in[base[lo]:base[lo] + size, cols], preferred_element_type=F32).astype(BF16)
        by_columns(write)

    def own_hot(at, d, k):
        hot[0:tok, at:at + LANES] = flag(iota((tok, LANES), 0) + me * tok == sels[d, k:k + 1, :]).astype(BF16)

    def toks_hot(at, toks):
        size = toks.shape[1]
        hot[0:tok, at:at + size] = flag(iota((tok, size), 0) + me * tok == toks[...]).astype(BF16)

    def rows_of(at, row, size, cols):
        return jnp.dot(hot[0:tok, at:at + size], rows_in[row:row + size, cols], preferred_element_type=F32)

    def give(c):
        size = sizes[c]
        depth = (SENT_AFTER[c] + 1) * cap
        for k in range(0, depth, LANES):
            part = min(LANES, depth - k)
            row = slots[me, k // LANES:k // LANES + 1, 0:part]
            hot[0:size, k:k + part] = flag(iota((size, part), 0) + off[c] == row).astype(BF16)

        def write(cols):
            packed = jnp.dot(hot[0:size, 0:depth], rows_in[own_at:own_at + depth, cols],
                             preferred_element_type=F32).astype(BF16)
            if c < XCHUNKS:
                packed = packed + out[off[c]:off[c + 1], cols]
            out[off[c]:off[c + 1], cols] = packed
        by_columns(write)
        link[c].start()

    def expert(e, carry):
        for j in range(XGROUPS):
            pl.when(e == X_FROM[j])(functools.partial(arrive, j))
        for j in range(2, XGROUPS):
            for c in range(X_LAST[j - 1] + 1, X_LAST[j] + 1):
                pl.when(e == X_FROM[j] - 1)(functools.partial(pass_on, c))
        for c in range(XCHUNKS, LATE - 1):
            pl.when(e == SENT_AFTER[c] + 6)(functools.partial(pass_on, c))
        rows = pl.ds(pl.multiple_of(e * cap, cap), cap)
        own = pl.ds(pl.multiple_of(own_at + e * cap, 32), cap)
        up_copy(e).wait()
        z = jnp.dot(picked[rows, :], up_buf[e % ring], preferred_element_type=F32)
        act = (0.5 * z * (1.0 + jnp.tanh(0.7978845608028654 * (z + 0.044715 * (z * z * z))))).astype(BF16)

        @pl.when(e + ring < experts)
        def _():
            up_copy(e + ring).start()

        down_copy(e).wait()
        for n in range(width // 512):
            cols = slice(n * 512, (n + 1) * 512)
            o = jnp.dot(act, down_buf[e % ring, :, cols], preferred_element_type=F32)
            rows_in[own, cols] = (o * gate_col[rows, :]).astype(BF16)

        @pl.when(e + ring < experts)
        def _():
            down_copy(e + ring).start()

        for c in range(FIRST, CHUNKS):
            pl.when(e == SENT_AFTER[c])(functools.partial(give, c))
        for j in range(GROUPS):
            pl.when(e == j * per_group + per_group - 1)(pass_near[j].start)
        return carry

    lax.fori_loop(0, experts, expert, 0)

    pass_on(LATE - 1)
    start = near_at[0]
    for k in range(GROUPS):
        own_hot(near_at[k] - start, near, k)
        own_hot(own_at + k * LANES - start, me, k)
    toks_hot(base[FIRST] - start, toks_a)
    toks_hot(base[XCHUNKS] - start, toks_b)
    for copy in pass_near + forward[XCHUNKS:LATE]:
        copy.wait_recv()

    def add_early(cols):
        acc[:, cols] = x_chip[own_rows, cols].astype(F32) + rows_of(0, start, base[LATE] - start, cols)
    by_columns(add_early)

    for c in range(LATE, CHUNKS):
        pass_on(c)
    toks_hot(0, toks_c)
    for c in range(LATE, CHUNKS):
        forward[c].wait_recv()

    def add_last(cols):
        y_ref[:, cols] = (acc[:, cols] + rows_of(0, base[LATE], base[CHUNKS] - base[LATE], cols)).astype(BF16)
    by_columns(add_last)

    if checked:
        ok_send.wait()
        ok_ref[0, 0] = jnp.min(ok_mine[...] * ok_other[...])
    else:
        ok_ref[0, 0] = 1.0
    to_near.wait_send()
    for copy in sel_send + link + forward + pass_near:
        copy.wait_send()


def solution(mesh):
    def layer(sizes, ring, step, checked, collective_id, sel, gate, x_loc, up_loc, down_loc):
        tok, width = x_loc.shape
        experts, _, hidden = up_loc.shape
        off, base, own_at, near_at = plan(sizes)
        vmem = pl.BlockSpec(memory_space=pltpu.VMEM)
        hbm = pl.BlockSpec(memory_space=pl.ANY)
        dma = pltpu.SemaphoreType.DMA
        each = dma((CHUNKS,))
        return pl.pallas_call(
            functools.partial(moe_kernel, sizes, ring, step, checked),
            out_shape=(jax.ShapeDtypeStruct((tok, width), BF16), jax.ShapeDtypeStruct((1, 1), F32)),
            in_specs=[vmem, vmem, hbm, hbm, hbm],
            out_specs=(vmem, pl.BlockSpec(memory_space=pltpu.SMEM)),
            scratch_shapes=[
                pltpu.VMEM((2 * tok, width), BF16),
                pltpu.VMEM((off[CHUNKS], width), BF16),
                pltpu.VMEM((base[CHUNKS], width), BF16),
                pltpu.VMEM((ENTRIES, width), BF16),
                pltpu.VMEM((tok, width), F32),
                pltpu.VMEM((tok, max(2 * tok, lanes(base[LATE] - near_at[0]))), BF16),
                pltpu.VMEM((GROUPS, LANES), I32),
                pltpu.VMEM((4, GROUPS, LANES), I32),
                pltpu.VMEM((4, GROUPS, LANES), I32),
                pltpu.VMEM((1, 2 * (off[XCHUNKS] - off[FIRST])), I32),
                pltpu.VMEM((1, 2 * (off[LATE] - off[XCHUNKS])), I32),
                pltpu.VMEM((1, 2 * (off[CHUNKS] - off[LATE])), I32),
                pltpu.VMEM((ENTRIES, 1), I32),
                pltpu.VMEM((ENTRIES, 1), F32),
                pltpu.VMEM((ENTRIES, 1), I32),
                pltpu.VMEM((8, LANES), I32),
                pltpu.VMEM((LANES, LANES), F32),
                pltpu.VMEM((8, LANES), F32),
                pltpu.VMEM((8, LANES), F32),
                pltpu.VMEM((ring, width, hidden), BF16),
                pltpu.VMEM((ring, hidden, width), BF16),
                dma, dma((ring,)), dma((ring,)), dma((3,)), dma((3,)), dma, dma,
                each, each, each, each, dma((GROUPS,)), dma((GROUPS,)), dma, dma,
            ],
            compiler_params=pltpu.CompilerParams(collective_id=collective_id, has_side_effects=True,
                                                 vmem_limit_bytes=56 * 1024 * 1024),
        )(sel, gate, x_loc, up_loc, down_loc)

    def local_layer(x_loc, sel_loc, gate_loc, up_loc, down_loc):
        args = (sel_loc, gate_loc, x_loc, up_loc, down_loc)
        y, ok = layer(*FIT.values(), 0, *args)
        return lax.cond(ok[0, 0] > 0.5, lambda: y, lambda: layer(*FULL.values(), 1, *args)[0])

    row_spec = P(("dp", "ep"), None)
    weight_spec = P("ep", None, None)
    return jax.shard_map(local_layer, mesh=mesh, in_specs=(row_spec, row_spec, row_spec, weight_spec, weight_spec), out_specs=row_spec, check_vma=False)
```

```python
import functools

import jax
import jax.numpy as jnp
from jax import lax
from jax.experimental import pallas as pl
from jax.experimental.pallas import tpu as pltpu
from jax.sharding import PartitionSpec as P

MESH = pl.DeviceIdType.MESH
GROUPS = 4
LANES = 128
ENTRIES = GROUPS * LANES
BF16 = jnp.bfloat16
F32 = jnp.float32
I32 = jnp.int32
SENT_AFTER = (None, None, None, None, 1, 3, 5, 7, 9, 11, 13, 15)
CHUNKS = len(SENT_AFTER)
FIRST = 4
X_FROM = (0, 2, 4, 6, 8, 12, 16)
X_LAST = (0, 1, 2, 3, 4, 6)
XGROUPS = len(X_LAST)
XCHUNKS = X_LAST[-1] + 1
LATE = CHUNKS - 2
FIT = dict(sizes=(64, 48, 32, 32, 48, 32, 48, 48, 48, 48, 64, 64), ring=4, step=2048, checked=True)
FULL = dict(sizes=(64, 64, 64, 64, 128, 64, 64, 192, 128, 64, 64, 64), ring=2, step=512, checked=False)


def iota(shape, dim):
    return lax.broadcasted_iota(I32, shape, dim)


def mm(a, b):
    return jnp.dot(a.astype(BF16), b.astype(BF16), preferred_element_type=F32)


def mm_t(a, b):
    return lax.dot_general(a.astype(BF16), b.astype(BF16), (((1,), (1,)), ((), ())), preferred_element_type=F32)


def flag(cond):
    return jnp.where(cond, 1.0, 0.0)


def total(a):
    return jnp.sum(jnp.sum(a, axis=1, keepdims=True), axis=0, keepdims=True)


def plan(sizes):
    off = [sum(sizes[:c]) for c in range(CHUNKS + 1)]
    near_at = [2 * off[FIRST] + j * LANES for j in range(GROUPS - 1)]
    shift = (GROUPS - 1) * LANES
    own_at = 2 * off[XCHUNKS] + shift
    near_at.append(own_at + ENTRIES)
    base = [2 * off[c] + (0 if c < FIRST else shift if c < XCHUNKS else shift + ENTRIES + LANES) for c in range(CHUNKS + 1)]
    return off, base, own_at, near_at


def lanes(n):
    return -(-n // LANES) * LANES


def moe_kernel(sizes, ring, step, checked, sel_in, gate_in, x_hbm, up_hbm, down_hbm, y_ref, ok_ref,
               x_chip, out, rows_in, picked, acc, hot,
               sel_row, sels, slots, toks_a, toks_b, toks_c, sel_col, gate_col, need_col, pos_out, square, ok_mine, ok_other,
               up_buf, down_buf,
               x_sem, up_sem, down_sem, send_sel, recv_sel, send_x, recv_x, send_link, recv_link, send_fwd, recv_fwd,
               send_near, recv_near, send_ok, recv_ok):
    tok, width = y_ref.shape
    experts, cap = sel_in.shape
    per_group = experts // GROUPS
    off, base, own_at, near_at = plan(sizes)
    me = lax.axis_index("ep")
    core = me % 2
    chip = me // 2
    near = me + 1 - 2 * core
    far = (me + 2) % 4
    diag = 3 - me
    peers = (near, far, diag)
    other_group = 1 - lax.axis_index("dp")

    def up_copy(e):
        return pltpu.make_async_copy(up_hbm.at[e], up_buf.at[e % ring], up_sem.at[e % ring])

    def down_copy(e):
        return pltpu.make_async_copy(down_hbm.at[e], down_buf.at[e % ring], down_sem.at[e % ring])

    def remote(src, dst, send, recv, peer, axis="ep"):
        return pltpu.make_async_remote_copy(src_ref=src, dst_ref=dst, send_sem=send, recv_sem=recv,
                                            device_id={axis: peer}, device_id_type=MESH)

    def by_columns(write, start=0, stop=width):
        if step == width:
            write(slice(start, stop))
        else:
            @pl.loop(start // step, stop // step)
            def _(n):
                write(pl.ds(pl.multiple_of(n * step, step), step))

    own_rows = pl.ds(pl.multiple_of(core * tok, tok), tok)
    load_x = pltpu.make_async_copy(x_hbm, x_chip.at[own_rows], x_sem)
    load_x.start()

    barrier = pltpu.get_barrier_semaphore()
    for peer in peers:
        pl.semaphore_signal(barrier, inc=1, device_id={"ep": peer}, device_id_type=MESH)
    if checked:
        pl.semaphore_signal(barrier, inc=1, device_id={"dp": other_group}, device_id_type=MESH)
    for e in range(ring):
        up_copy(e).start()
        down_copy(e).start()

    spread = flag(iota((cap, LANES), 0) == iota((cap, LANES), 1) % cap)
    inside = flag(iota((experts, LANES), 0) % per_group == iota((experts, LANES), 1) // cap)
    gather = flag(iota((GROUPS, experts), 1) // per_group == iota((GROUPS, experts), 0))
    high = mm(gather, mm((sel_in[...] >> 5).astype(F32), spread) * inside)
    low = mm(gather, mm((sel_in[...] & 31).astype(F32), spread) * inside)
    sel_row[...] = (high * 32.0 + low).astype(I32)
    pl.semaphore_wait(barrier, 4 if checked else 3)
    sel_send = [remote(sel_row, sels.at[me], send_sel.at[i], recv_sel.at[i], peer) for i, peer in enumerate(peers)]
    for copy in sel_send:
        copy.start()
    load_x.wait()
    halves = [slice(h * width // 2, (h + 1) * width // 2) for h in range(2)]
    to_near = []
    for h, cols in enumerate(halves):
        block = x_chip.at[own_rows, pl.ds(cols.start, width // 2)]
        to_near.append(remote(block, block, send_x.at[h], recv_x.at[h], near))
        to_near[h].start()
    sels[me] = sel_row[...]
    square[...] = jnp.zeros_like(square)
    square[0:experts, 0:cap] = sel_in[...].astype(F32)
    square[experts:2 * experts, 0:cap] = gate_in[...]
    turned = square[...].T
    for e in range(experts):
        sel_col[e * cap:(e + 1) * cap, :] = turned[0:cap, e:e + 1].astype(I32)
        gate_col[e * cap:(e + 1) * cap, :] = turned[0:cap, experts + e:experts + e + 1]

    before = flag(iota((LANES, LANES), 0) < iota((LANES, LANES), 1))
    ones = jnp.ones((LANES, LANES), F32)
    rows_before = flag(iota((XGROUPS * 8, XGROUPS * 8), 1) < iota((XGROUPS * 8, XGROUPS * 8), 0))
    for copy in sel_send:
        copy.wait_recv()

    def row_order(c):
        start = (1 - c) * (2 * tok)
        seen = jnp.zeros((8, LANES), F32)
        firsts, fit = [], jnp.ones((1, 1), F32)
        lane = iota((1, 2 * LANES), 1) % LANES
        for j in range(XGROUPS):
            k = X_FROM[j] * cap // LANES
            row = jnp.concatenate([sels[2 * c, k:k + 1, :], sels[2 * c + 1, k:k + 1, :]], axis=1) - start
            if X_FROM[j + 1] - X_FROM[j] < per_group:
                from_lane = (X_FROM[j] % per_group) * cap
                row = jnp.where((lane >= from_lane) & (lane < from_lane + (X_FROM[j + 1] - X_FROM[j]) * cap), row, -1)
            row_high = flag(iota((8, 2 * LANES), 0) == (row >> 7))
            row_low = flag(iota((LANES, 2 * LANES), 0) == (row & 127))
            need = flag(mm_t(row_high, row_low) > 0.5)
            firsts.append(need * (1.0 - seen))
            seen = jnp.maximum(seen, need)
            fit = fit * flag(total(seen) < 2.0 * off[X_LAST[j] + 1] + 0.5)
        first = jnp.concatenate(firsts, axis=0)
        place = mm(first, before) + mm(rows_before, mm(first, ones))
        pos = sum(firsts[j] * (place[8 * j:8 * j + 8] + 1.0) for j in range(XGROUPS)) - 1.0
        return pos.astype(I32), total(seen), fit

    def entry_order(d, sent_rows):
        away = flag((sels[d] >> 10) != d // 2)
        rank = mm(away, before)
        lane = iota((GROUPS, LANES), 1)
        early = flag(lane < LANES // 2)
        count = jnp.sum(away, axis=1, keepdims=True)
        count_early = jnp.sum(away * early, axis=1, keepdims=True)
        end = jnp.floor((sent_rows + 1.0) * 0.5)
        for j in range(GROUPS):
            row = slice(j, j + 1)
            begin = jnp.maximum(end, float(off[FIRST + 2 * j]))
            later = jnp.maximum(begin + count_early[row], float(off[FIRST + 2 * j + 1]))
            place = rank[row] + jnp.where(lane[row] < LANES // 2, begin, later - count_early[row])
            end = later + count[row] - count_early[row]
            slots[d, row, :] = (away[row] * (place + 1.0) - 1.0).astype(I32)
        return flag(end < off[CHUNKS] + 0.5)

    pos, rows_sent, fit = row_order(1 - chip)
    pos_out[...] = jnp.where((pos & 1) == core, pos >> 1, -1)

    def pack_hot(lo, hi):
        size = off[hi] - off[lo]
        for b in range(8):
            hot[0:size, b * LANES:(b + 1) * LANES] = flag(iota((size, LANES), 0) + off[lo] == pos_out[b:b + 1, :]).astype(BF16)

    def pack(skip, lo, hi, start=0, stop=width):
        size = off[hi] - off[lo]

        def write(cols):
            out[off[lo]:off[hi], cols] = jnp.dot(hot[skip:skip + size, 0:2 * tok], x_chip[:, cols],
                                                 preferred_element_type=F32).astype(BF16)
        by_columns(write, start, stop)

    link, link0, forward = [], [], []
    for c in range(CHUNKS):
        mine = rows_in.at[pl.ds(base[c], sizes[c])]
        theirs = rows_in.at[pl.ds(base[c] + sizes[c], sizes[c])]
        if c == 0:
            for h, cols in enumerate(halves):
                part = pl.ds(cols.start, width // 2)
                link0.append(remote(out.at[pl.ds(0, sizes[0]), part], rows_in.at[pl.ds(base[0], sizes[0]), part],
                                    send_link.at[h * CHUNKS], recv_link.at[h * CHUNKS], far))
        link.append(link0 if c == 0 else [
            remote(out.at[pl.ds(off[c], sizes[c])], mine, send_link.at[c], recv_link.at[c], far)])
        forward.append(remote(mine, theirs, send_fwd.at[c], recv_fwd.at[c], near))
    pass_near = []
    for j in range(GROUPS):
        pass_near.append(remote(rows_in.at[pl.ds(own_at + j * LANES, LANES)], rows_in.at[pl.ds(near_at[j], LANES)],
                                send_near.at[j], recv_near.at[j], near))

    pack_hot(0, FIRST)
    to_near[0].wait_recv()
    pack(0, 0, 1, halves[0].start, halves[0].stop)
    link0[0].start()
    to_near[1].wait_recv()
    pack(0, 0, 1, halves[1].start, halves[1].stop)
    link0[1].start()
    pack(off[1], 1, FIRST)
    for c in range(1, FIRST):
        link[c][0].start()
    pack_hot(FIRST, XCHUNKS)
    pack(0, FIRST, XCHUNKS)

    wanted, rows_got, fit_in = row_order(chip)
    fit = fit * fit_in
    for d in range(4):
        same_chip = flag(jnp.full((1, 1), d // 2, I32) == chip)
        fit = fit * entry_order(d, same_chip * rows_sent + (1.0 - same_chip) * rows_got)

    slot = wanted >> 1
    side = jnp.where((wanted & 1) == core, 0, 1)
    where_in = jnp.full((8, LANES), -1, I32)
    for c in range(XCHUNKS):
        here = (slot >= off[c]) & (slot < off[c + 1]) & (wanted >= 0)
        where_in = jnp.where(here, base[c] - off[c] + slot + side * sizes[c], where_in)
    where_in = where_in.astype(F32)
    found = jnp.zeros((ENTRIES, LANES), F32)
    for b in range(8):
        start = (1 - chip) * (2 * tok) + b * LANES
        found = found + jnp.where(sel_col[...] == iota((ENTRIES, LANES), 1) + start, where_in[b:b + 1, :] + 1.0, 0.0)
    need_col[...] = (jnp.sum(found, axis=1, keepdims=True) - 1.0).astype(I32)

    for b in range(8):
        start = chip * (2 * tok) + b * LANES
        hot[0:ENTRIES, b * LANES:(b + 1) * LANES] = flag(sel_col[...] == iota((ENTRIES, LANES), 1) + start).astype(BF16)

    def pick_local(cols):
        picked[:, cols] = jnp.dot(hot[0:ENTRIES, 0:2 * tok], x_chip[:, cols], preferred_element_type=F32).astype(BF16)
    by_columns(pick_local)

    values = []
    for d in (far, diag):
        for k in range(GROUPS):
            at = iota((8, LANES), 0)
            row = sels[d, k:k + 1, :]
            values.append(jnp.where(at == 0, row >> 5, jnp.where(at == 1, row & 31, 1)).astype(F32))
    values = jnp.concatenate(values, axis=1)
    for c in range(FIRST, CHUNKS):
        size = sizes[c]
        at = iota((2 * size, LANES), 0)
        for f, d in enumerate((far, diag)):
            key = jnp.where((at >= f * size) & (at < (f + 1) * size), at - f * size + off[c], -2)
            for k in range(GROUPS):
                block = (f * GROUPS + k) * LANES
                hot[0:2 * size, block:block + LANES] = flag(key == slots[d, k:k + 1, :]).astype(BF16)
        sums = mm_t(values, hot[0:2 * size, 0:2 * ENTRIES])
        token = jnp.where(sums[2:3] > 0.5, sums[0:1] * 32.0 + sums[1:2], -1.0).astype(I32)
        toks, start = (toks_a, FIRST) if c < XCHUNKS else (toks_b, XCHUNKS) if c < LATE else (toks_c, LATE)
        at = base[c] - base[start]
        toks[:, at:at + 2 * size] = token

    if checked:
        ok_mine[...] = jnp.broadcast_to(fit, ok_mine.shape)
        ok_send = remote(ok_mine, ok_other, send_ok, recv_ok, other_group, "dp")
        ok_send.start()

    def pass_on(c):
        for copy in link[c]:
            copy.wait_recv()
        forward[c].start()

    def arrive(j):
        r0, lo, hi = X_FROM[j] * cap, (X_LAST[j - 1] + 1 if j else 0), X_LAST[j] + 1
        size = base[hi - 1] + 2 * sizes[hi - 1] - base[lo]
        if j < 2:
            pass_on(lo)
        hot[r0:ENTRIES, 0:size] = flag(need_col[r0:, :] == iota((ENTRIES - r0, size), 1) + base[lo]).astype(BF16)
        for c in range(lo, hi):
            forward[c].wait_recv()

        def write(cols):
            picked[r0:, cols] = picked[r0:, cols] + jnp.dot(
                hot[r0:ENTRIES, 0:size], rows_in[base[lo]:base[lo] + size, cols], preferred_element_type=F32).astype(BF16)
        by_columns(write)

    def own_hot(at, d, k):
        hot[0:tok, at:at + LANES] = flag(iota((tok, LANES), 0) + me * tok == sels[d, k:k + 1, :]).astype(BF16)

    def toks_hot(at, toks):
        size = toks.shape[1]
        hot[0:tok, at:at + size] = flag(iota((tok, size), 0) + me * tok == toks[...]).astype(BF16)

    def rows_of(at, row, size, cols):
        return jnp.dot(hot[0:tok, at:at + size], rows_in[row:row + size, cols], preferred_element_type=F32)

    def give(c):
        size = sizes[c]
        depth = (SENT_AFTER[c] + 1) * cap
        for k in range(0, depth, LANES):
            part = min(LANES, depth - k)
            row = slots[me, k // LANES:k // LANES + 1, 0:part]
            hot[0:size, k:k + part] = flag(iota((size, part), 0) + off[c] == row).astype(BF16)

        def write(cols):
            packed = jnp.dot(hot[0:size, 0:depth], rows_in[own_at:own_at + depth, cols],
                             preferred_element_type=F32).astype(BF16)
            if c < XCHUNKS:
                packed = packed + out[off[c]:off[c + 1], cols]
            out[off[c]:off[c + 1], cols] = packed
        by_columns(write)
        link[c][0].start()

    def expert(e, carry):
        for j in range(XGROUPS):
            pl.when(e == X_FROM[j])(functools.partial(arrive, j))
        for j in range(2, XGROUPS):
            for c in range(X_LAST[j - 1] + 1, X_LAST[j] + 1):
                pl.when(e == X_FROM[j] - 1)(functools.partial(pass_on, c))
        for c in range(XCHUNKS, LATE - 1):
            pl.when(e == SENT_AFTER[c] + 6)(functools.partial(pass_on, c))
        rows = pl.ds(pl.multiple_of(e * cap, cap), cap)
        own = pl.ds(pl.multiple_of(own_at + e * cap, 32), cap)
        up_copy(e).wait()
        z = jnp.dot(picked[rows, :], up_buf[e % ring], preferred_element_type=F32)
        act = (0.5 * z * (1.0 + jnp.tanh(0.7978845608028654 * (z + 0.044715 * (z * z * z))))).astype(BF16)

        @pl.when(e + ring < experts)
        def _():
            up_copy(e + ring).start()

        down_copy(e).wait()
        for n in range(width // 512):
            cols = slice(n * 512, (n + 1) * 512)
            o = jnp.dot(act, down_buf[e % ring, :, cols], preferred_element_type=F32)
            rows_in[own, cols] = (o * gate_col[rows, :]).astype(BF16)

        @pl.when(e + ring < experts)
        def _():
            down_copy(e + ring).start()

        for c in range(FIRST, CHUNKS):
            pl.when(e == SENT_AFTER[c])(functools.partial(give, c))
        for j in range(GROUPS):
            pl.when(e == j * per_group + per_group - 1)(pass_near[j].start)
        return carry

    lax.fori_loop(0, experts, expert, 0)

    pass_on(LATE - 1)
    start = near_at[0]
    for k in range(GROUPS):
        own_hot(near_at[k] - start, near, k)
        own_hot(own_at + k * LANES - start, me, k)
    toks_hot(base[FIRST] - start, toks_a)
    toks_hot(base[XCHUNKS] - start, toks_b)
    for copy in pass_near + forward[XCHUNKS:LATE]:
        copy.wait_recv()

    def add_early(cols):
        acc[:, cols] = x_chip[own_rows, cols].astype(F32) + rows_of(0, start, base[LATE] - start, cols)
    by_columns(add_early)

    for c in range(LATE, CHUNKS):
        pass_on(c)
    toks_hot(0, toks_c)
    for c in range(LATE, CHUNKS):
        forward[c].wait_recv()

    def add_last(cols):
        y_ref[:, cols] = (acc[:, cols] + rows_of(0, base[LATE], base[CHUNKS] - base[LATE], cols)).astype(BF16)
    by_columns(add_last)

    if checked:
        ok_send.wait()
        ok_ref[0, 0] = jnp.min(ok_mine[...] * ok_other[...])
    else:
        ok_ref[0, 0] = 1.0
    for copy in to_near + sel_send + sum(link, []) + forward + pass_near:
        copy.wait_send()


def solution(mesh):
    def layer(sizes, ring, step, checked, collective_id, sel, gate, x_loc, up_loc, down_loc):
        tok, width = x_loc.shape
        experts, _, hidden = up_loc.shape
        off, base, own_at, near_at = plan(sizes)
        vmem = pl.BlockSpec(memory_space=pltpu.VMEM)
        hbm = pl.BlockSpec(memory_space=pl.ANY)
        dma = pltpu.SemaphoreType.DMA
        each = dma((CHUNKS,))
        return pl.pallas_call(
            functools.partial(moe_kernel, sizes, ring, step, checked),
            out_shape=(jax.ShapeDtypeStruct((tok, width), BF16), jax.ShapeDtypeStruct((1, 1), F32)),
            in_specs=[vmem, vmem, hbm, hbm, hbm],
            out_specs=(vmem, pl.BlockSpec(memory_space=pltpu.SMEM)),
            scratch_shapes=[
                pltpu.VMEM((2 * tok, width), BF16),
                pltpu.VMEM((off[CHUNKS], width), BF16),
                pltpu.VMEM((base[CHUNKS], width), BF16),
                pltpu.VMEM((ENTRIES, width), BF16),
                pltpu.VMEM((tok, width), F32),
                pltpu.VMEM((tok, max(2 * tok, lanes(base[LATE] - near_at[0]))), BF16),
                pltpu.VMEM((GROUPS, LANES), I32),
                pltpu.VMEM((4, GROUPS, LANES), I32),
                pltpu.VMEM((4, GROUPS, LANES), I32),
                pltpu.VMEM((1, 2 * (off[XCHUNKS] - off[FIRST])), I32),
                pltpu.VMEM((1, 2 * (off[LATE] - off[XCHUNKS])), I32),
                pltpu.VMEM((1, 2 * (off[CHUNKS] - off[LATE])), I32),
                pltpu.VMEM((ENTRIES, 1), I32),
                pltpu.VMEM((ENTRIES, 1), F32),
                pltpu.VMEM((ENTRIES, 1), I32),
                pltpu.VMEM((8, LANES), I32),
                pltpu.VMEM((LANES, LANES), F32),
                pltpu.VMEM((8, LANES), F32),
                pltpu.VMEM((8, LANES), F32),
                pltpu.VMEM((ring, width, hidden), BF16),
                pltpu.VMEM((ring, hidden, width), BF16),
                dma, dma((ring,)), dma((ring,)), dma((3,)), dma((3,)), dma((2,)), dma((2,)),
                dma((CHUNKS + 1,)), dma((CHUNKS + 1,)), each, each, dma((GROUPS,)), dma((GROUPS,)), dma, dma,
            ],
            compiler_params=pltpu.CompilerParams(collective_id=collective_id, has_side_effects=True,
                                                 vmem_limit_bytes=58 * 1024 * 1024),
        )(sel, gate, x_loc, up_loc, down_loc)

    def local_layer(x_loc, sel_loc, gate_loc, up_loc, down_loc):
        args = (sel_loc, gate_loc, x_loc, up_loc, down_loc)
        y, ok = layer(*FIT.values(), 0, *args)
        return lax.cond(ok[0, 0] > 0.5, lambda: y, lambda: layer(*FULL.values(), 1, *args)[0])

    row_spec = P(("dp", "ep"), None)
    weight_spec = P("ep", None, None)
    return jax.shard_map(local_layer, mesh=mesh, in_specs=(row_spec, row_spec, row_spec, weight_spec, weight_spec), out_specs=row_spec, check_vma=False)
```

```python
import functools

import jax
import jax.numpy as jnp
from jax import lax
from jax.experimental import pallas as pl
from jax.experimental.pallas import tpu as pltpu
from jax.sharding import PartitionSpec as P

MESH = pl.DeviceIdType.MESH
GROUPS = 4
LANES = 128
ENTRIES = GROUPS * LANES
BF16 = jnp.bfloat16
F32 = jnp.float32
I32 = jnp.int32
SENT_AFTER = (None, None, None, 1, 3, 5, 7, 9, 11, 13, 14, 15)
CHUNKS = len(SENT_AFTER)
FIRST = 3
X_FROM = (0, 2, 4, 6, 8, 12, 16)
X_LAST = (0, 1, 2, 3, 4, 5)
XGROUPS = len(X_LAST)
XCHUNKS = X_LAST[-1] + 1
LATE = CHUNKS - 3
FIT = dict(sizes=(64, 48, 32, 48, 32, 48, 48, 48, 48, 48, 32, 48), ring=4, step=2048, checked=True)
FULL = dict(sizes=(64, 64, 64, 64, 128, 128, 192, 128, 64, 64, 32, 32), ring=2, step=512, checked=False)


def iota(shape, dim):
    return lax.broadcasted_iota(I32, shape, dim)


def mm(a, b):
    return jnp.dot(a.astype(BF16), b.astype(BF16), preferred_element_type=F32)


def mm_t(a, b):
    return lax.dot_general(a.astype(BF16), b.astype(BF16), (((1,), (1,)), ((), ())), preferred_element_type=F32)


def flag(cond):
    return jnp.where(cond, 1.0, 0.0)


def total(a):
    return jnp.sum(jnp.sum(a, axis=1, keepdims=True), axis=0, keepdims=True)


def plan(sizes):
    off = [sum(sizes[:c]) for c in range(CHUNKS + 1)]
    near_at = [2 * off[FIRST] + j * LANES for j in range(GROUPS - 1)]
    shift = (GROUPS - 1) * LANES
    own_at = 2 * off[XCHUNKS] + shift
    near_at.append(own_at + ENTRIES)
    base = [2 * off[c] + (0 if c < FIRST else shift if c < XCHUNKS else shift + ENTRIES + LANES) for c in range(CHUNKS + 1)]
    return off, base, own_at, near_at


def lanes(n):
    return -(-n // LANES) * LANES


def moe_kernel(sizes, ring, step, checked, sel_in, gate_in, x_hbm, up_hbm, down_hbm, y_ref, ok_ref,
               x_chip, out, rows_in, picked, acc, hot,
               sel_row, sels, slots, toks_a, toks_b, toks_c, sel_col, gate_col, need_col, pos_out, square, ok_mine, ok_other,
               up_buf, down_buf,
               x_sem, up_sem, down_sem, send_sel, recv_sel, send_x, recv_x, send_link, recv_link, send_fwd, recv_fwd,
               send_near, recv_near, send_ok, recv_ok):
    tok, width = y_ref.shape
    experts, cap = sel_in.shape
    per_group = experts // GROUPS
    off, base, own_at, near_at = plan(sizes)
    me = lax.axis_index("ep")
    core = me % 2
    chip = me // 2
    near = me + 1 - 2 * core
    far = (me + 2) % 4
    diag = 3 - me
    peers = (near, far, diag)
    other_group = 1 - lax.axis_index("dp")

    def up_copy(e):
        return pltpu.make_async_copy(up_hbm.at[e], up_buf.at[e % ring], up_sem.at[e % ring])

    def down_copy(e):
        return pltpu.make_async_copy(down_hbm.at[e], down_buf.at[e % ring], down_sem.at[e % ring])

    def remote(src, dst, send, recv, peer, axis="ep"):
        return pltpu.make_async_remote_copy(src_ref=src, dst_ref=dst, send_sem=send, recv_sem=recv,
                                            device_id={axis: peer}, device_id_type=MESH)

    def by_columns(write, start=0, stop=width):
        if step == width:
            write(slice(start, stop))
        else:
            @pl.loop(start // step, stop // step)
            def _(n):
                write(pl.ds(pl.multiple_of(n * step, step), step))

    own_rows = pl.ds(pl.multiple_of(core * tok, tok), tok)
    load_x = pltpu.make_async_copy(x_hbm, x_chip.at[own_rows], x_sem)
    load_x.start()

    barrier = pltpu.get_barrier_semaphore()
    for peer in peers:
        pl.semaphore_signal(barrier, inc=1, device_id={"ep": peer}, device_id_type=MESH)
    if checked:
        pl.semaphore_signal(barrier, inc=1, device_id={"dp": other_group}, device_id_type=MESH)
    for e in range(ring):
        up_copy(e).start()
        down_copy(e).start()

    spread = flag(iota((cap, LANES), 0) == iota((cap, LANES), 1) % cap)
    inside = flag(iota((experts, LANES), 0) % per_group == iota((experts, LANES), 1) // cap)
    gather = flag(iota((GROUPS, experts), 1) // per_group == iota((GROUPS, experts), 0))
    high = mm(gather, mm((sel_in[...] >> 5).astype(F32), spread) * inside)
    low = mm(gather, mm((sel_in[...] & 31).astype(F32), spread) * inside)
    sel_row[...] = (high * 32.0 + low).astype(I32)
    pl.semaphore_wait(barrier, 4 if checked else 3)
    sel_send = [remote(sel_row, sels.at[me], send_sel.at[i], recv_sel.at[i], peer) for i, peer in enumerate(peers)]
    for copy in sel_send:
        copy.start()
    load_x.wait()
    halves = [slice(h * width // 2, (h + 1) * width // 2) for h in range(2)]
    to_near = []
    for h, cols in enumerate(halves):
        block = x_chip.at[own_rows, pl.ds(cols.start, width // 2)]
        to_near.append(remote(block, block, send_x.at[h], recv_x.at[h], near))
        to_near[h].start()
    sels[me] = sel_row[...]
    square[...] = jnp.zeros_like(square)
    square[0:experts, 0:cap] = sel_in[...].astype(F32)
    square[experts:2 * experts, 0:cap] = gate_in[...]
    turned = square[...].T
    for e in range(experts):
        sel_col[e * cap:(e + 1) * cap, :] = turned[0:cap, e:e + 1].astype(I32)
        gate_col[e * cap:(e + 1) * cap, :] = turned[0:cap, experts + e:experts + e + 1]

    before = flag(iota((LANES, LANES), 0) < iota((LANES, LANES), 1))
    ones = jnp.ones((LANES, LANES), F32)
    rows_before = flag(iota((XGROUPS * 8, XGROUPS * 8), 1) < iota((XGROUPS * 8, XGROUPS * 8), 0))
    for copy in sel_send:
        copy.wait_recv()

    def row_order(c):
        start = (1 - c) * (2 * tok)
        seen = jnp.zeros((8, LANES), F32)
        firsts, fit = [], jnp.ones((1, 1), F32)
        lane = iota((1, 2 * LANES), 1) % LANES
        for j in range(XGROUPS):
            k = X_FROM[j] * cap // LANES
            row = jnp.concatenate([sels[2 * c, k:k + 1, :], sels[2 * c + 1, k:k + 1, :]], axis=1) - start
            if X_FROM[j + 1] - X_FROM[j] < per_group:
                from_lane = (X_FROM[j] % per_group) * cap
                row = jnp.where((lane >= from_lane) & (lane < from_lane + (X_FROM[j + 1] - X_FROM[j]) * cap), row, -1)
            row_high = flag(iota((8, 2 * LANES), 0) == (row >> 7))
            row_low = flag(iota((LANES, 2 * LANES), 0) == (row & 127))
            need = flag(mm_t(row_high, row_low) > 0.5)
            firsts.append(need * (1.0 - seen))
            seen = jnp.maximum(seen, need)
            fit = fit * flag(total(seen) < 2.0 * off[X_LAST[j] + 1] + 0.5)
        first = jnp.concatenate(firsts, axis=0)
        place = mm(first, before) + mm(rows_before, mm(first, ones))
        pos = sum(firsts[j] * (place[8 * j:8 * j + 8] + 1.0) for j in range(XGROUPS)) - 1.0
        return pos.astype(I32), total(seen), fit

    def entry_order(d, sent_rows):
        away = flag((sels[d] >> 10) != d // 2)
        rank = mm(away, before)
        lane = iota((1, LANES), 1)
        end = jnp.floor((sent_rows + 1.0) * 0.5)
        stop = 0
        for c in range(FIRST, CHUNKS):
            start, stop = stop, (SENT_AFTER[c] + 1) * cap
            row = slice(start // LANES, start // LANES + 1)
            lo, hi = start % LANES, start % LANES + stop - start
            if lo == 0:
                earlier, place = jnp.zeros((1, 1), F32), jnp.zeros((1, LANES), F32)
            here = (lane >= lo) & (lane < hi)
            count = jnp.sum(jnp.where(here, away[row], 0.0), axis=1, keepdims=True)
            begin = jnp.maximum(end, float(off[c]))
            place = jnp.where(here, rank[row] - earlier + begin, place)
            earlier = earlier + count
            end = begin + count
            if hi == LANES:
                slots[d, row, :] = (away[row] * (place + 1.0) - 1.0).astype(I32)
        return flag(end < off[CHUNKS] + 0.5)

    pos, rows_sent, fit = row_order(1 - chip)
    pos_out[...] = jnp.where((pos & 1) == core, pos >> 1, -1)

    def pack_hot(lo, hi):
        size = off[hi] - off[lo]
        for b in range(8):
            hot[0:size, b * LANES:(b + 1) * LANES] = flag(iota((size, LANES), 0) + off[lo] == pos_out[b:b + 1, :]).astype(BF16)

    def pack(skip, lo, hi, start=0, stop=width):
        size = off[hi] - off[lo]

        def write(cols):
            out[off[lo]:off[hi], cols] = jnp.dot(hot[skip:skip + size, 0:2 * tok], x_chip[:, cols],
                                                 preferred_element_type=F32).astype(BF16)
        by_columns(write, start, stop)

    link, link0, forward = [], [], []
    for c in range(CHUNKS):
        mine = rows_in.at[pl.ds(base[c], sizes[c])]
        theirs = rows_in.at[pl.ds(base[c] + sizes[c], sizes[c])]
        if c == 0:
            for h, cols in enumerate(halves):
                part = pl.ds(cols.start, width // 2)
                link0.append(remote(out.at[pl.ds(0, sizes[0]), part], rows_in.at[pl.ds(base[0], sizes[0]), part],
                                    send_link.at[h * CHUNKS], recv_link.at[h * CHUNKS], far))
        link.append(link0 if c == 0 else [
            remote(out.at[pl.ds(off[c], sizes[c])], mine, send_link.at[c], recv_link.at[c], far)])
        forward.append(remote(mine, theirs, send_fwd.at[c], recv_fwd.at[c], near))
    pass_near = []
    for j in range(GROUPS):
        pass_near.append(remote(rows_in.at[pl.ds(own_at + j * LANES, LANES)], rows_in.at[pl.ds(near_at[j], LANES)],
                                send_near.at[j], recv_near.at[j], near))

    pack_hot(0, FIRST)
    to_near[0].wait_recv()
    pack(0, 0, 1, halves[0].start, halves[0].stop)
    link0[0].start()
    to_near[1].wait_recv()
    pack(0, 0, 1, halves[1].start, halves[1].stop)
    link0[1].start()
    pack(off[1], 1, FIRST)
    for c in range(1, FIRST):
        link[c][0].start()
    pack_hot(FIRST, XCHUNKS)
    pack(0, FIRST, XCHUNKS)

    wanted, rows_got, fit_in = row_order(chip)
    fit = fit * fit_in
    for d in range(4):
        same_chip = flag(jnp.full((1, 1), d // 2, I32) == chip)
        fit = fit * entry_order(d, same_chip * rows_sent + (1.0 - same_chip) * rows_got)

    slot = wanted >> 1
    side = jnp.where((wanted & 1) == core, 0, 1)
    where_in = jnp.full((8, LANES), -1, I32)
    for c in range(XCHUNKS):
        here = (slot >= off[c]) & (slot < off[c + 1]) & (wanted >= 0)
        where_in = jnp.where(here, base[c] - off[c] + slot + side * sizes[c], where_in)
    where_in = where_in.astype(F32)
    found = jnp.zeros((ENTRIES, LANES), F32)
    for b in range(8):
        start = (1 - chip) * (2 * tok) + b * LANES
        found = found + jnp.where(sel_col[...] == iota((ENTRIES, LANES), 1) + start, where_in[b:b + 1, :] + 1.0, 0.0)
    need_col[...] = (jnp.sum(found, axis=1, keepdims=True) - 1.0).astype(I32)

    for b in range(8):
        start = chip * (2 * tok) + b * LANES
        hot[0:ENTRIES, b * LANES:(b + 1) * LANES] = flag(sel_col[...] == iota((ENTRIES, LANES), 1) + start).astype(BF16)

    def pick_local(cols):
        picked[:, cols] = jnp.dot(hot[0:ENTRIES, 0:2 * tok], x_chip[:, cols], preferred_element_type=F32).astype(BF16)
    by_columns(pick_local)

    values = []
    for d in (far, diag):
        for k in range(GROUPS):
            at = iota((8, LANES), 0)
            row = sels[d, k:k + 1, :]
            values.append(jnp.where(at == 0, row >> 5, jnp.where(at == 1, row & 31, 1)).astype(F32))
    values = jnp.concatenate(values, axis=1)
    for c in range(FIRST, CHUNKS):
        size = sizes[c]
        at = iota((2 * size, LANES), 0)
        for f, d in enumerate((far, diag)):
            key = jnp.where((at >= f * size) & (at < (f + 1) * size), at - f * size + off[c], -2)
            for k in range(GROUPS):
                block = (f * GROUPS + k) * LANES
                hot[0:2 * size, block:block + LANES] = flag(key == slots[d, k:k + 1, :]).astype(BF16)
        sums = mm_t(values, hot[0:2 * size, 0:2 * ENTRIES])
        token = jnp.where(sums[2:3] > 0.5, sums[0:1] * 32.0 + sums[1:2], -1.0).astype(I32)
        toks, start = (toks_a, FIRST) if c < XCHUNKS else (toks_b, XCHUNKS) if c < LATE else (toks_c, LATE)
        at = base[c] - base[start]
        toks[:, at:at + 2 * size] = token

    if checked:
        ok_mine[...] = jnp.broadcast_to(fit, ok_mine.shape)
        ok_send = remote(ok_mine, ok_other, send_ok, recv_ok, other_group, "dp")
        ok_send.start()

    def pass_on(c):
        for copy in link[c]:
            copy.wait_recv()
        forward[c].start()

    def arrive(j):
        r0, lo, hi = X_FROM[j] * cap, (X_LAST[j - 1] + 1 if j else 0), X_LAST[j] + 1
        size = base[hi - 1] + 2 * sizes[hi - 1] - base[lo]
        if j < 2:
            pass_on(lo)
        hot[r0:ENTRIES, 0:size] = flag(need_col[r0:, :] == iota((ENTRIES - r0, size), 1) + base[lo]).astype(BF16)
        for c in range(lo, hi):
            forward[c].wait_recv()

        def write(cols):
            picked[r0:, cols] = picked[r0:, cols] + jnp.dot(
                hot[r0:ENTRIES, 0:size], rows_in[base[lo]:base[lo] + size, cols], preferred_element_type=F32).astype(BF16)
        by_columns(write)

    def own_hot(at, d, k):
        hot[0:tok, at:at + LANES] = flag(iota((tok, LANES), 0) + me * tok == sels[d, k:k + 1, :]).astype(BF16)

    def toks_hot(at, toks):
        size = toks.shape[1]
        hot[0:tok, at:at + size] = flag(iota((tok, size), 0) + me * tok == toks[...]).astype(BF16)

    def rows_of(at, row, size, cols):
        return jnp.dot(hot[0:tok, at:at + size], rows_in[row:row + size, cols], preferred_element_type=F32)

    def give(c):
        size = sizes[c]
        depth = (SENT_AFTER[c] + 1) * cap
        for k in range(0, depth, LANES):
            part = min(LANES, depth - k)
            row = slots[me, k // LANES:k // LANES + 1, 0:part]
            hot[0:size, k:k + part] = flag(iota((size, part), 0) + off[c] == row).astype(BF16)

        def write(cols):
            packed = jnp.dot(hot[0:size, 0:depth], rows_in[own_at:own_at + depth, cols],
                             preferred_element_type=F32).astype(BF16)
            if c < XCHUNKS:
                packed = packed + out[off[c]:off[c + 1], cols]
            out[off[c]:off[c + 1], cols] = packed
        by_columns(write)
        link[c][0].start()

    def expert(e, carry):
        for j in range(XGROUPS):
            pl.when(e == X_FROM[j])(functools.partial(arrive, j))
        for j in range(2, XGROUPS):
            for c in range(X_LAST[j - 1] + 1, X_LAST[j] + 1):
                pl.when(e == X_FROM[j] - 1)(functools.partial(pass_on, c))
        for c in range(XCHUNKS, LATE - 1):
            pl.when(e == SENT_AFTER[c] + 6)(functools.partial(pass_on, c))
        rows = pl.ds(pl.multiple_of(e * cap, cap), cap)
        own = pl.ds(pl.multiple_of(own_at + e * cap, 32), cap)
        up_copy(e).wait()
        down_copy(e).wait()
        z = jnp.dot(picked[rows, :], up_buf[e % ring], preferred_element_type=F32)
        act = (0.5 * z * (1.0 + jnp.tanh(0.7978845608028654 * (z + 0.044715 * (z * z * z))))).astype(BF16)

        @pl.when(e + ring < experts)
        def _():
            up_copy(e + ring).start()

        for n in range(width // 512):
            cols = slice(n * 512, (n + 1) * 512)
            o = jnp.dot(act, down_buf[e % ring, :, cols], preferred_element_type=F32)
            rows_in[own, cols] = (o * gate_col[rows, :]).astype(BF16)

        @pl.when(e + ring < experts)
        def _():
            down_copy(e + ring).start()

        for c in range(FIRST, CHUNKS):
            pl.when(e == SENT_AFTER[c])(functools.partial(give, c))
        for j in range(GROUPS):
            pl.when(e == j * per_group + per_group - 1)(pass_near[j].start)
        return carry

    lax.fori_loop(0, experts, expert, 0)

    pass_on(LATE - 1)
    start = near_at[0]
    for k in range(GROUPS):
        own_hot(near_at[k] - start, near, k)
        own_hot(own_at + k * LANES - start, me, k)
    toks_hot(base[FIRST] - start, toks_a)
    toks_hot(base[XCHUNKS] - start, toks_b)
    for copy in pass_near + forward[XCHUNKS:LATE]:
        copy.wait_recv()

    def add_early(cols):
        acc[:, cols] = x_chip[own_rows, cols].astype(F32) + rows_of(0, start, base[LATE] - start, cols)
    by_columns(add_early)

    for c in range(LATE, CHUNKS):
        pass_on(c)
    toks_hot(0, toks_c)
    for c in range(LATE, CHUNKS):
        forward[c].wait_recv()

    def add_last(cols):
        y_ref[:, cols] = (acc[:, cols] + rows_of(0, base[LATE], base[CHUNKS] - base[LATE], cols)).astype(BF16)
    by_columns(add_last)

    if checked:
        ok_send.wait()
        ok_ref[0, 0] = jnp.min(ok_mine[...] * ok_other[...])
    else:
        ok_ref[0, 0] = 1.0
    for copy in to_near + sel_send + sum(link, []) + forward + pass_near:
        copy.wait_send()


def solution(mesh):
    def layer(sizes, ring, step, checked, collective_id, sel, gate, x_loc, up_loc, down_loc):
        tok, width = x_loc.shape
        experts, _, hidden = up_loc.shape
        off, base, own_at, near_at = plan(sizes)
        vmem = pl.BlockSpec(memory_space=pltpu.VMEM)
        hbm = pl.BlockSpec(memory_space=pl.ANY)
        dma = pltpu.SemaphoreType.DMA
        each = dma((CHUNKS,))
        return pl.pallas_call(
            functools.partial(moe_kernel, sizes, ring, step, checked),
            out_shape=(jax.ShapeDtypeStruct((tok, width), BF16), jax.ShapeDtypeStruct((1, 1), F32)),
            in_specs=[vmem, vmem, hbm, hbm, hbm],
            out_specs=(vmem, pl.BlockSpec(memory_space=pltpu.SMEM)),
            scratch_shapes=[
                pltpu.VMEM((2 * tok, width), BF16),
                pltpu.VMEM((off[CHUNKS], width), BF16),
                pltpu.VMEM((base[CHUNKS], width), BF16),
                pltpu.VMEM((ENTRIES, width), BF16),
                pltpu.VMEM((tok, width), F32),
                pltpu.VMEM((tok, max(2 * tok, lanes(base[LATE] - near_at[0]))), BF16),
                pltpu.VMEM((GROUPS, LANES), I32),
                pltpu.VMEM((4, GROUPS, LANES), I32),
                pltpu.VMEM((4, GROUPS, LANES), I32),
                pltpu.VMEM((1, 2 * (off[XCHUNKS] - off[FIRST])), I32),
                pltpu.VMEM((1, 2 * (off[LATE] - off[XCHUNKS])), I32),
                pltpu.VMEM((1, 2 * (off[CHUNKS] - off[LATE])), I32),
                pltpu.VMEM((ENTRIES, 1), I32),
                pltpu.VMEM((ENTRIES, 1), F32),
                pltpu.VMEM((ENTRIES, 1), I32),
                pltpu.VMEM((8, LANES), I32),
                pltpu.VMEM((LANES, LANES), F32),
                pltpu.VMEM((8, LANES), F32),
                pltpu.VMEM((8, LANES), F32),
                pltpu.VMEM((ring, width, hidden), BF16),
                pltpu.VMEM((ring, hidden, width), BF16),
                dma, dma((ring,)), dma((ring,)), dma((3,)), dma((3,)), dma((2,)), dma((2,)),
                dma((CHUNKS + 1,)), dma((CHUNKS + 1,)), each, each, dma((GROUPS,)), dma((GROUPS,)), dma, dma,
            ],
            compiler_params=pltpu.CompilerParams(collective_id=collective_id, has_side_effects=True,
                                                 vmem_limit_bytes=58 * 1024 * 1024),
        )(sel, gate, x_loc, up_loc, down_loc)

    def local_layer(x_loc, sel_loc, gate_loc, up_loc, down_loc):
        args = (sel_loc, gate_loc, x_loc, up_loc, down_loc)
        y, ok = layer(*FIT.values(), 0, *args)
        return lax.cond(ok[0, 0] > 0.5, lambda: y, lambda: layer(*FULL.values(), 1, *args)[0])

    row_spec = P(("dp", "ep"), None)
    weight_spec = P("ep", None, None)
    return jax.shard_map(local_layer, mesh=mesh, in_specs=(row_spec, row_spec, row_spec, weight_spec, weight_spec), out_specs=row_spec, check_vma=False)
```

```python
import functools

import jax
import jax.numpy as jnp
from jax import lax
from jax.experimental import pallas as pl
from jax.experimental.pallas import tpu as pltpu
from jax.sharding import PartitionSpec as P

MESH = pl.DeviceIdType.MESH
GROUPS = 4
LANES = 128
ENTRIES = GROUPS * LANES
BF16 = jnp.bfloat16
F32 = jnp.float32
I32 = jnp.int32
SENT_AFTER = (None, None, None, 1, 3, 5, 7, 9, 11, 13, 14, 15)
CHUNKS = len(SENT_AFTER)
FIRST = 3
X_FROM = (0, 2, 4, 6, 8, 12, 16)
X_LAST = (0, 1, 2, 3, 4, 5)
XGROUPS = len(X_LAST)
XCHUNKS = X_LAST[-1] + 1
LATE = CHUNKS - 3
FIT = dict(sizes=(64, 48, 32, 48, 32, 48, 48, 48, 48, 48, 32, 48), ring=4, step=2048, checked=True)
FULL = dict(sizes=(64, 64, 64, 64, 128, 128, 192, 128, 64, 64, 32, 32), ring=2, step=512, checked=False)


def iota(shape, dim):
    return lax.broadcasted_iota(I32, shape, dim)


def mm(a, b):
    return jnp.dot(a.astype(BF16), b.astype(BF16), preferred_element_type=F32)


def mm_t(a, b):
    return lax.dot_general(a.astype(BF16), b.astype(BF16), (((1,), (1,)), ((), ())), preferred_element_type=F32)


def flag(cond):
    return jnp.where(cond, 1.0, 0.0)


def total(a):
    return jnp.sum(jnp.sum(a, axis=1, keepdims=True), axis=0, keepdims=True)


def plan(sizes):
    off = [sum(sizes[:c]) for c in range(CHUNKS + 1)]
    near_at = [2 * off[FIRST] + j * LANES for j in range(GROUPS - 1)]
    shift = (GROUPS - 1) * LANES
    own_at = 2 * off[XCHUNKS] + shift
    near_at.append(own_at + ENTRIES)
    base = [2 * off[c] + (0 if c < FIRST else shift if c < XCHUNKS else shift + ENTRIES + LANES) for c in range(CHUNKS + 1)]
    return off, base, own_at, near_at


def lanes(n):
    return -(-n // LANES) * LANES


def moe_kernel(sizes, ring, step, checked, sel_in, gate_in, x_hbm, up_hbm, down_hbm, y_ref, ok_ref,
               x_chip, out, rows_in, picked, acc, hot,
               sel_row, sels, slots, toks_a, toks_b, toks_c, sel_col, gate_col, need_col, pos_out, square, ok_mine, ok_other,
               up_buf, down_buf,
               x_sem, up_sem, down_sem, send_sel, recv_sel, send_x, recv_x, send_link, recv_link, send_fwd, recv_fwd,
               send_near, recv_near, send_ok, recv_ok):
    tok, width = y_ref.shape
    experts, cap = sel_in.shape
    per_group = experts // GROUPS
    off, base, own_at, near_at = plan(sizes)
    me = lax.axis_index("ep")
    core = me % 2
    chip = me // 2
    near = me + 1 - 2 * core
    far = (me + 2) % 4
    diag = 3 - me
    peers = (near, far, diag)
    other_group = 1 - lax.axis_index("dp")

    def up_copy(e):
        return pltpu.make_async_copy(up_hbm.at[e], up_buf.at[e % ring], up_sem.at[e % ring])

    def down_copy(e):
        return pltpu.make_async_copy(down_hbm.at[e], down_buf.at[e % ring], down_sem.at[e % ring])

    def remote(src, dst, send, recv, peer, axis="ep"):
        return pltpu.make_async_remote_copy(src_ref=src, dst_ref=dst, send_sem=send, recv_sem=recv,
                                            device_id={axis: peer}, device_id_type=MESH)

    def by_columns(write, start=0, stop=width):
        if step == width:
            write(slice(start, stop))
        else:
            @pl.loop(start // step, stop // step)
            def _(n):
                write(pl.ds(pl.multiple_of(n * step, step), step))

    own_rows = pl.ds(pl.multiple_of(core * tok, tok), tok)
    load_x = pltpu.make_async_copy(x_hbm, x_chip.at[own_rows], x_sem)
    load_x.start()

    barrier = pltpu.get_barrier_semaphore()
    for peer in peers:
        pl.semaphore_signal(barrier, inc=1, device_id={"ep": peer}, device_id_type=MESH)
    if checked:
        pl.semaphore_signal(barrier, inc=1, device_id={"dp": other_group}, device_id_type=MESH)
    for e in range(ring):
        up_copy(e).start()
        down_copy(e).start()

    spread = flag(iota((cap, LANES), 0) == iota((cap, LANES), 1) % cap)
    inside = flag(iota((experts, LANES), 0) % per_group == iota((experts, LANES), 1) // cap)
    gather = flag(iota((GROUPS, experts), 1) // per_group == iota((GROUPS, experts), 0))
    high = mm(gather, mm((sel_in[...] >> 5).astype(F32), spread) * inside)
    low = mm(gather, mm((sel_in[...] & 31).astype(F32), spread) * inside)
    sel_row[...] = (high * 32.0 + low).astype(I32)
    pl.semaphore_wait(barrier, 4 if checked else 3)
    sel_send = [remote(sel_row, sels.at[me], send_sel.at[i], recv_sel.at[i], peer) for i, peer in enumerate(peers)]
    for copy in sel_send:
        copy.start()
    load_x.wait()
    halves = [slice(h * width // 2, (h + 1) * width // 2) for h in range(2)]
    to_near = []
    for h, cols in enumerate(halves):
        block = x_chip.at[own_rows, pl.ds(cols.start, width // 2)]
        to_near.append(remote(block, block, send_x.at[h], recv_x.at[h], near))
        to_near[h].start()
    sels[me] = sel_row[...]
    square[...] = jnp.zeros_like(square)
    square[0:experts, 0:cap] = sel_in[...].astype(F32)
    square[experts:2 * experts, 0:cap] = gate_in[...]
    turned = square[...].T
    for e in range(experts):
        sel_col[e * cap:(e + 1) * cap, :] = turned[0:cap, e:e + 1].astype(I32)
        gate_col[e * cap:(e + 1) * cap, :] = turned[0:cap, experts + e:experts + e + 1]

    before = flag(iota((LANES, LANES), 0) < iota((LANES, LANES), 1))
    ones = jnp.ones((LANES, LANES), F32)
    rows_before = flag(iota((XGROUPS * 8, XGROUPS * 8), 1) < iota((XGROUPS * 8, XGROUPS * 8), 0))
    for copy in sel_send:
        copy.wait_recv()

    def row_order(c):
        start = (1 - c) * (2 * tok)
        seen = jnp.zeros((8, LANES), F32)
        firsts, fit = [], jnp.ones((1, 1), F32)
        lane = iota((1, 2 * LANES), 1) % LANES
        for j in range(XGROUPS):
            k = X_FROM[j] * cap // LANES
            row = jnp.concatenate([sels[2 * c, k:k + 1, :], sels[2 * c + 1, k:k + 1, :]], axis=1) - start
            if X_FROM[j + 1] - X_FROM[j] < per_group:
                from_lane = (X_FROM[j] % per_group) * cap
                row = jnp.where((lane >= from_lane) & (lane < from_lane + (X_FROM[j + 1] - X_FROM[j]) * cap), row, -1)
            row_high = flag(iota((8, 2 * LANES), 0) == (row >> 7))
            row_low = flag(iota((LANES, 2 * LANES), 0) == (row & 127))
            need = flag(mm_t(row_high, row_low) > 0.5)
            firsts.append(need * (1.0 - seen))
            seen = jnp.maximum(seen, need)
            fit = fit * flag(total(seen) < 2.0 * off[X_LAST[j] + 1] + 0.5)
        first = jnp.concatenate(firsts, axis=0)
        place = mm(first, before) + mm(rows_before, mm(first, ones))
        pos = sum(firsts[j] * (place[8 * j:8 * j + 8] + 1.0) for j in range(XGROUPS)) - 1.0
        return pos.astype(I32), total(seen), fit

    def entry_order(d, sent_rows):
        away = flag((sels[d] >> 10) != d // 2)
        rank = mm(away, before)
        lane = iota((1, LANES), 1)
        end = jnp.floor((sent_rows + 1.0) * 0.5)
        stop = 0
        for c in range(FIRST, CHUNKS):
            start, stop = stop, (SENT_AFTER[c] + 1) * cap
            row = slice(start // LANES, start // LANES + 1)
            lo, hi = start % LANES, start % LANES + stop - start
            if lo == 0:
                earlier, place = jnp.zeros((1, 1), F32), jnp.zeros((1, LANES), F32)
            here = (lane >= lo) & (lane < hi)
            count = jnp.sum(jnp.where(here, away[row], 0.0), axis=1, keepdims=True)
            begin = jnp.maximum(end, float(off[c]))
            place = jnp.where(here, rank[row] - earlier + begin, place)
            earlier = earlier + count
            end = begin + count
            if hi == LANES:
                slots[d, row, :] = (away[row] * (place + 1.0) - 1.0).astype(I32)
        return flag(end < off[CHUNKS] + 0.5)

    pos, rows_sent, fit = row_order(1 - chip)
    pos_out[...] = jnp.where((pos & 1) == core, pos >> 1, -1)

    def pack_hot(lo, hi):
        size = off[hi] - off[lo]
        for b in range(8):
            hot[0:size, b * LANES:(b + 1) * LANES] = flag(iota((size, LANES), 0) + off[lo] == pos_out[b:b + 1, :]).astype(BF16)

    def pack(skip, lo, hi, start=0, stop=width):
        size = off[hi] - off[lo]

        def write(cols):
            out[off[lo]:off[hi], cols] = jnp.dot(hot[skip:skip + size, 0:2 * tok], x_chip[:, cols],
                                                 preferred_element_type=F32).astype(BF16)
        by_columns(write, start, stop)

    link, link0, forward = [], [], []
    for c in range(CHUNKS):
        mine = rows_in.at[pl.ds(base[c], sizes[c])]
        theirs = rows_in.at[pl.ds(base[c] + sizes[c], sizes[c])]
        if c == 0:
            for h, cols in enumerate(halves):
                part = pl.ds(cols.start, width // 2)
                link0.append(remote(out.at[pl.ds(0, sizes[0]), part], rows_in.at[pl.ds(base[0], sizes[0]), part],
                                    send_link.at[h * CHUNKS], recv_link.at[h * CHUNKS], far))
        link.append(link0 if c == 0 else [
            remote(out.at[pl.ds(off[c], sizes[c])], mine, send_link.at[c], recv_link.at[c], far)])
        forward.append(remote(mine, theirs, send_fwd.at[c], recv_fwd.at[c], near))
    pass_near = []
    for j in range(GROUPS):
        pass_near.append(remote(rows_in.at[pl.ds(own_at + j * LANES, LANES)], rows_in.at[pl.ds(near_at[j], LANES)],
                                send_near.at[j], recv_near.at[j], near))

    pack_hot(0, FIRST)
    to_near[0].wait_recv()
    pack(0, 0, 1, halves[0].start, halves[0].stop)
    link0[0].start()
    to_near[1].wait_recv()
    pack(0, 0, 1, halves[1].start, halves[1].stop)
    link0[1].start()
    pack(off[1], 1, FIRST)
    for c in range(1, FIRST):
        link[c][0].start()
    pack_hot(FIRST, XCHUNKS)
    pack(0, FIRST, XCHUNKS)

    wanted, rows_got, fit_in = row_order(chip)
    fit = fit * fit_in
    for d in range(4):
        same_chip = flag(jnp.full((1, 1), d // 2, I32) == chip)
        fit = fit * entry_order(d, same_chip * rows_sent + (1.0 - same_chip) * rows_got)

    slot = wanted >> 1
    side = jnp.where((wanted & 1) == core, 0, 1)
    where_in = jnp.full((8, LANES), -1, I32)
    for c in range(XCHUNKS):
        here = (slot >= off[c]) & (slot < off[c + 1]) & (wanted >= 0)
        where_in = jnp.where(here, base[c] - off[c] + slot + side * sizes[c], where_in)
    where_in = where_in.astype(F32)
    found = jnp.zeros((ENTRIES, LANES), F32)
    for b in range(8):
        start = (1 - chip) * (2 * tok) + b * LANES
        found = found + jnp.where(sel_col[...] == iota((ENTRIES, LANES), 1) + start, where_in[b:b + 1, :] + 1.0, 0.0)
    need_col[...] = (jnp.sum(found, axis=1, keepdims=True) - 1.0).astype(I32)

    for b in range(8):
        start = chip * (2 * tok) + b * LANES
        hot[0:ENTRIES, b * LANES:(b + 1) * LANES] = flag(sel_col[...] == iota((ENTRIES, LANES), 1) + start).astype(BF16)

    def pick_local(cols):
        picked[:, cols] = jnp.dot(hot[0:ENTRIES, 0:2 * tok], x_chip[:, cols], preferred_element_type=F32).astype(BF16)
    by_columns(pick_local)

    def tokens(first, last):
        values = []
        for d in (far, diag):
            for k in range(GROUPS):
                at = iota((8, LANES), 0)
                row = sels[d, k:k + 1, :]
                values.append(jnp.where(at == 0, row >> 5, jnp.where(at == 1, row & 31, 1)).astype(F32))
        values = jnp.concatenate(values, axis=1)
        for c in range(first, last):
            size = sizes[c]
            at = iota((2 * size, LANES), 0)
            for f, d in enumerate((far, diag)):
                key = jnp.where((at >= f * size) & (at < (f + 1) * size), at - f * size + off[c], -2)
                for k in range(GROUPS):
                    block = (f * GROUPS + k) * LANES
                    hot[0:2 * size, block:block + LANES] = flag(key == slots[d, k:k + 1, :]).astype(BF16)
            sums = mm_t(values, hot[0:2 * size, 0:2 * ENTRIES])
            token = jnp.where(sums[2:3] > 0.5, sums[0:1] * 32.0 + sums[1:2], -1.0).astype(I32)
            toks, start = (toks_a, FIRST) if c < XCHUNKS else (toks_b, XCHUNKS) if c < LATE else (toks_c, LATE)
            at = base[c] - base[start]
            toks[:, at:at + 2 * size] = token

    tokens(FIRST, LATE)

    if checked:
        ok_mine[...] = jnp.broadcast_to(fit, ok_mine.shape)
        ok_send = remote(ok_mine, ok_other, send_ok, recv_ok, other_group, "dp")
        ok_send.start()

    def pass_on(c):
        for copy in link[c]:
            copy.wait_recv()
        forward[c].start()

    def arrive(j):
        r0, lo, hi = X_FROM[j] * cap, (X_LAST[j - 1] + 1 if j else 0), X_LAST[j] + 1
        size = base[hi - 1] + 2 * sizes[hi - 1] - base[lo]
        if j < 2:
            pass_on(lo)
        if j == 0:
            tokens(LATE, CHUNKS)
        hot[r0:ENTRIES, 0:size] = flag(need_col[r0:, :] == iota((ENTRIES - r0, size), 1) + base[lo]).astype(BF16)
        for c in range(lo, hi):
            forward[c].wait_recv()

        def write(cols):
            picked[r0:, cols] = picked[r0:, cols] + jnp.dot(
                hot[r0:ENTRIES, 0:size], rows_in[base[lo]:base[lo] + size, cols], preferred_element_type=F32).astype(BF16)
        by_columns(write)

    def own_hot(at, d, k):
        hot[0:tok, at:at + LANES] = flag(iota((tok, LANES), 0) + me * tok == sels[d, k:k + 1, :]).astype(BF16)

    def toks_hot(at, toks):
        size = toks.shape[1]
        hot[0:tok, at:at + size] = flag(iota((tok, size), 0) + me * tok == toks[...]).astype(BF16)

    def rows_of(at, row, size, cols):
        return jnp.dot(hot[0:tok, at:at + size], rows_in[row:row + size, cols], preferred_element_type=F32)

    def give(c):
        size = sizes[c]
        depth = (SENT_AFTER[c] + 1) * cap
        for k in range(0, depth, LANES):
            part = min(LANES, depth - k)
            row = slots[me, k // LANES:k // LANES + 1, 0:part]
            hot[0:size, k:k + part] = flag(iota((size, part), 0) + off[c] == row).astype(BF16)

        def write(cols):
            packed = jnp.dot(hot[0:size, 0:depth], rows_in[own_at:own_at + depth, cols],
                             preferred_element_type=F32).astype(BF16)
            if c < XCHUNKS:
                packed = packed + out[off[c]:off[c + 1], cols]
            out[off[c]:off[c + 1], cols] = packed
        by_columns(write)
        link[c][0].start()

    def expert(e, carry):
        for j in range(XGROUPS):
            pl.when(e == X_FROM[j])(functools.partial(arrive, j))
        for j in range(2, XGROUPS):
            for c in range(X_LAST[j - 1] + 1, X_LAST[j] + 1):
                pl.when(e == X_FROM[j] - 1)(functools.partial(pass_on, c))
        for c in range(XCHUNKS, LATE - 1):
            pl.when(e == SENT_AFTER[c] + 6)(functools.partial(pass_on, c))
        rows = pl.ds(pl.multiple_of(e * cap, cap), cap)
        own = pl.ds(pl.multiple_of(own_at + e * cap, 32), cap)
        up_copy(e).wait()
        down_copy(e).wait()
        z = jnp.dot(picked[rows, :], up_buf[e % ring], preferred_element_type=F32)
        act = (0.5 * z * (1.0 + jnp.tanh(0.7978845608028654 * (z + 0.044715 * (z * z * z))))).astype(BF16)

        @pl.when(e + ring < experts)
        def _():
            up_copy(e + ring).start()

        for n in range(width // 512):
            cols = slice(n * 512, (n + 1) * 512)
            o = jnp.dot(act, down_buf[e % ring, :, cols], preferred_element_type=F32)
            rows_in[own, cols] = (o * gate_col[rows, :]).astype(BF16)

        @pl.when(e + ring < experts)
        def _():
            down_copy(e + ring).start()

        for c in range(FIRST, CHUNKS):
            pl.when(e == SENT_AFTER[c])(functools.partial(give, c))
        for j in range(GROUPS):
            pl.when(e == j * per_group + per_group - 1)(pass_near[j].start)
        return carry

    lax.fori_loop(0, experts, expert, 0)

    pass_on(LATE - 1)
    start = near_at[0]
    for k in range(GROUPS):
        own_hot(near_at[k] - start, near, k)
        own_hot(own_at + k * LANES - start, me, k)
    toks_hot(base[FIRST] - start, toks_a)
    toks_hot(base[XCHUNKS] - start, toks_b)
    for copy in pass_near + forward[XCHUNKS:LATE]:
        copy.wait_recv()

    def add_early(cols):
        acc[:, cols] = x_chip[own_rows, cols].astype(F32) + rows_of(0, start, base[LATE] - start, cols)
    by_columns(add_early)

    for c in range(LATE, CHUNKS):
        pass_on(c)
    toks_hot(0, toks_c)
    for c in range(LATE, CHUNKS):
        forward[c].wait_recv()

    def add_last(cols):
        y_ref[:, cols] = (acc[:, cols] + rows_of(0, base[LATE], base[CHUNKS] - base[LATE], cols)).astype(BF16)
    by_columns(add_last)

    if checked:
        ok_send.wait()
        ok_ref[0, 0] = jnp.min(ok_mine[...] * ok_other[...])
    else:
        ok_ref[0, 0] = 1.0
    for copy in to_near + sel_send + sum(link, []) + forward + pass_near:
        copy.wait_send()


def solution(mesh):
    def layer(sizes, ring, step, checked, collective_id, sel, gate, x_loc, up_loc, down_loc):
        tok, width = x_loc.shape
        experts, _, hidden = up_loc.shape
        off, base, own_at, near_at = plan(sizes)
        vmem = pl.BlockSpec(memory_space=pltpu.VMEM)
        hbm = pl.BlockSpec(memory_space=pl.ANY)
        dma = pltpu.SemaphoreType.DMA
        each = dma((CHUNKS,))
        return pl.pallas_call(
            functools.partial(moe_kernel, sizes, ring, step, checked),
            out_shape=(jax.ShapeDtypeStruct((tok, width), BF16), jax.ShapeDtypeStruct((1, 1), F32)),
            in_specs=[vmem, vmem, hbm, hbm, hbm],
            out_specs=(vmem, pl.BlockSpec(memory_space=pltpu.SMEM)),
            scratch_shapes=[
                pltpu.VMEM((2 * tok, width), BF16),
                pltpu.VMEM((off[CHUNKS], width), BF16),
                pltpu.VMEM((base[CHUNKS], width), BF16),
                pltpu.VMEM((ENTRIES, width), BF16),
                pltpu.VMEM((tok, width), F32),
                pltpu.VMEM((tok, max(2 * tok, lanes(base[LATE] - near_at[0]))), BF16),
                pltpu.VMEM((GROUPS, LANES), I32),
                pltpu.VMEM((4, GROUPS, LANES), I32),
                pltpu.VMEM((4, GROUPS, LANES), I32),
                pltpu.VMEM((1, 2 * (off[XCHUNKS] - off[FIRST])), I32),
                pltpu.VMEM((1, 2 * (off[LATE] - off[XCHUNKS])), I32),
                pltpu.VMEM((1, 2 * (off[CHUNKS] - off[LATE])), I32),
                pltpu.VMEM((ENTRIES, 1), I32),
                pltpu.VMEM((ENTRIES, 1), F32),
                pltpu.VMEM((ENTRIES, 1), I32),
                pltpu.VMEM((8, LANES), I32),
                pltpu.VMEM((LANES, LANES), F32),
                pltpu.VMEM((8, LANES), F32),
                pltpu.VMEM((8, LANES), F32),
                pltpu.VMEM((ring, width, hidden), BF16),
                pltpu.VMEM((ring, hidden, width), BF16),
                dma, dma((ring,)), dma((ring,)), dma((3,)), dma((3,)), dma((2,)), dma((2,)),
                dma((CHUNKS + 1,)), dma((CHUNKS + 1,)), each, each, dma((GROUPS,)), dma((GROUPS,)), dma, dma,
            ],
            compiler_params=pltpu.CompilerParams(collective_id=collective_id, has_side_effects=True,
                                                 vmem_limit_bytes=58 * 1024 * 1024),
        )(sel, gate, x_loc, up_loc, down_loc)

    def local_layer(x_loc, sel_loc, gate_loc, up_loc, down_loc):
        args = (sel_loc, gate_loc, x_loc, up_loc, down_loc)
        y, ok = layer(*FIT.values(), 0, *args)
        return lax.cond(ok[0, 0] > 0.5, lambda: y, lambda: layer(*FULL.values(), 1, *args)[0])

    row_spec = P(("dp", "ep"), None)
    weight_spec = P("ep", None, None)
    return jax.shard_map(local_layer, mesh=mesh, in_specs=(row_spec, row_spec, row_spec, weight_spec, weight_spec), out_specs=row_spec, check_vma=False)
```
